32 devices in a mesh: tm: 4 (over x, core), space: 8 (over z, y).
Axes of the slice: x: 2, y: 2, z: 4, core: 2. Of those that a mesh axis runs over, the one named last changes fastest.
Arguments:
- start_value: float32 [4, 8, 512, 256], P('tm', 'space'), may hold values from -6 to 6
- old_nodes: float32 [4, 3, 8, 512, 256], P('tm', None, 'space'), may hold values from -6 to 6
- diffusivity: float32 [8, 512, 256], P('space'), may hold values from 0.2 to 2
Outputs:
- fine_nodes: float32 [4, 3, 8, 512, 256], P('tm', None, 'space')
- next_start: float32 [4, 8, 512, 256], P('tm', 'space')
- next_coarse: float32 [4, 8, 512, 256], P('tm', 'space')
The draws below stay inside these ranges and needn't reach their ends.
All inputs are finite; a program needn't handle non-finite values.
Results may differ from the reference program's by a relative error of at most 0.0001.
Values sent between devices are 32-bit elements; how exact they have to be, the bound alone decides.
A program may use at most 64 MiB of HBM per device.

```python
import math
import jax
import jax.numpy as jnp
from jax import lax

NY = 512
NZ = 256
NODES = 3
CG_ITERS = 2
NX = 8
SLICES = 4


def shard_levels(key, extent, split, low, largest):
    factor_of = 1.0
    for dim, parts in split:
        heights = jax.random.uniform(jax.random.fold_in(jax.random.fold_in(key, 6), dim), (parts,), jnp.float32, low / len(split), largest / len(split))
        factor_of = factor_of * jnp.repeat(jnp.exp(heights), extent[dim] // parts).reshape((-1,) + (1,) * (len(extent) - 1 - dim))
    return factor_of


def bell_draw(own_key, shape, scale, most, cuts=(), kind=jnp.bfloat16):
    array = scale * jax.random.normal(own_key, shape, jnp.float32)
    if cuts:
        array = array * shard_levels(own_key, shape, cuts, -0.22, 0.18)
    return jnp.clip(array, -most, most).astype(kind)


def setup_inputs(seed: int = 0) -> dict:
    streams_of = jax.random.split(jax.random.key(seed), 4)
    start_value = bell_draw(streams_of[0], (SLICES, NX, NY, NZ), 1.0, 6.0, ((0, 4), (1, 8)), jnp.float32)
    old_nodes = bell_draw(streams_of[1], (SLICES, NODES, NX, NY, NZ), 1.0, 6.0, ((0, 4), (2, 8)), jnp.float32)
    diffusivity = jnp.clip(jnp.exp(math.log(2.0) - 2.3025851 * jax.random.uniform(streams_of[2], (NX, NY, NZ), jnp.float32) ** shard_levels(streams_of[2], (NX, NY, NZ), ((0, 8),), -0.2, 0.2)), 0.2, 2.0)
    return dict(start_value=start_value, old_nodes=old_nodes, diffusivity=diffusivity)


STEP = 2.0
ROOT_SIX = math.sqrt(6.0)
NODE_TIMES = [(4.0 - ROOT_SIX) / 10.0, (4.0 + ROOT_SIX) / 10.0, 1.0]
COLLOC = [[(88.0 - 7.0 * ROOT_SIX) / 360.0, (296.0 - 169.0 * ROOT_SIX) / 1800.0, (-2.0 + 3.0 * ROOT_SIX) / 225.0], [(296.0 + 169.0 * ROOT_SIX) / 1800.0, (88.0 + 7.0 * ROOT_SIX) / 360.0, (-2.0 - 3.0 * ROOT_SIX) / 225.0], [(16.0 - ROOT_SIX) / 36.0, (16.0 + ROOT_SIX) / 36.0, 1.0 / 9.0]]

def sweep_weight(row, column):
    below = COLLOC[row - 1][column] if row > 0 else 0.0
    return COLLOC[row][column] - below

def node_width(row):
    below = NODE_TIMES[row - 1] if row > 0 else 0.0
    return NODE_TIMES[row] - below

def neighbour(field, dim, forward):
    length = field.shape[dim]
    edge = jnp.zeros_like(lax.slice_in_dim(field, 0, 1, axis=dim))
    if forward:
        return jnp.concatenate([lax.slice_in_dim(field, 1, length, axis=dim), edge], axis=dim)
    return jnp.concatenate([edge, lax.slice_in_dim(field, 0, length - 1, axis=dim)], axis=dim)

def face_table(kappa):
    faces = []
    for dim in range(3):
        for forward in (True, False):
            faces.append(0.5 * (kappa + neighbour(kappa, dim, forward)))
    total = faces[0] + faces[1] + faces[2] + faces[3] + faces[4] + faces[5]
    return (faces, total)

def apply_heat(field, faces, total):
    result = faces[0] * neighbour(field, 0, True) + faces[1] * neighbour(field, 0, False)
    result = result + faces[2] * neighbour(field, 1, True) + faces[3] * neighbour(field, 1, False)
    result = result + faces[4] * neighbour(field, 2, True) + faces[5] * neighbour(field, 2, False)
    return result - total * field

def combine(weights, images):
    summed = weights[0] * images[0]
    for column in range(1, 3):
        summed = summed + weights[column] * images[column]
    return summed

def solve(guess, residual, width, faces, total):
    iterate = guess
    direction = residual
    norm_now = jnp.sum(residual * residual)
    for sweep in range(CG_ITERS):
        product = direction - width * apply_heat(direction, faces, total)
        step_size = norm_now / jnp.sum(direction * product)
        iterate = iterate + step_size * direction
        if sweep + 1 < CG_ITERS:
            residual = residual - step_size * product
            norm_next = jnp.sum(residual * residual)
            direction = residual + norm_next / norm_now * direction
            norm_now = norm_next
    return iterate

def reference(start_value, old_nodes, diffusivity):
    faces, total = face_table(diffusivity)

    def one_slice(pair):
        begin, previous_nodes = pair
        images = [apply_heat(previous_nodes[column], faces, total) for column in range(3)]
        previous = begin
        fresh = []
        for row in range(3):
            weights = [sweep_weight(row, column) for column in range(3)]
            residual = previous - previous_nodes[row] + STEP * combine(weights, images)
            result = solve(previous_nodes[row], residual, STEP * node_width(row), faces, total)
            fresh.append(result)
            previous = result
        coarse_res = begin - previous_nodes[2] + STEP * combine(COLLOC[2], images)
        coarse_end = solve(previous_nodes[2], coarse_res, STEP, faces, total)
        return (jnp.stack(fresh), coarse_end)
    fine_nodes, coarse_ends = lax.map(one_slice, (start_value, old_nodes))
    next_start = jnp.concatenate([start_value[:1], fine_nodes[:-1, 2]], axis=0)
    next_coarse = jnp.concatenate([start_value[:1], coarse_ends[:-1]], axis=0)
    return (fine_nodes, next_start, next_coarse)
```

```python
import math

import jax
import jax.numpy as jnp
from jax import lax
from jax.experimental import pallas as pl
from jax.experimental.pallas import tpu as pltpu
from jax.sharding import PartitionSpec as P

STEP = 2.0
ROOT_SIX = math.sqrt(6.0)
NODE_TIMES = [(4.0 - ROOT_SIX) / 10.0, (4.0 + ROOT_SIX) / 10.0, 1.0]
COLLOC = [
    [
        (88.0 - 7.0 * ROOT_SIX) / 360.0,
        (296.0 - 169.0 * ROOT_SIX) / 1800.0,
        (-2.0 + 3.0 * ROOT_SIX) / 225.0,
    ],
    [
        (296.0 + 169.0 * ROOT_SIX) / 1800.0,
        (88.0 + 7.0 * ROOT_SIX) / 360.0,
        (-2.0 - 3.0 * ROOT_SIX) / 225.0,
    ],
    [(16.0 - ROOT_SIX) / 36.0, (16.0 + ROOT_SIX) / 36.0, 1.0 / 9.0],
]
MESH = pl.DeviceIdType.MESH
PAD = 8

KAPPA, NODE, START, RES, IMG = 0, 1, 4, 5, 9
FIELDS = 13
H_KAPPA, H_NODE, H_RES, H_IMG = 0, 1, 4, 8
HALOS = 12


def sweep_weight(row, column):
    below = COLLOC[row - 1][column] if row > 0 else 0.0
    return COLLOC[row][column] - below


def node_width(row):
    below = NODE_TIMES[row - 1] if row > 0 else 0.0
    return NODE_TIMES[row] - below


WIDTHS = [STEP * node_width(0), STEP * node_width(1), STEP * node_width(2), STEP]


def tile_of(rows, most):
    best = 8
    for size in range(8, most + 1, 8):
        if rows % size == 0:
            best = size
    return best


def kernel(
    slices, slabs, ny, nz,
    start_in, nodes_in, kappa_in,
    fine_out, start_out, coarse_out,
    field, lower, upper, faces, across, image, base, result, staged, mail, sums,
    swap_s, swap_r, own_s, halo_s, halo_r, sum_s, sum_r, out_s, out_r, keep_s, end_s, end_r, copy_s,
):
    f32 = jnp.float32
    t = lax.axis_index("tm")
    s = lax.axis_index("space")
    h = lax.rem(s, 2)
    p = lax.div(s, 2)
    pairs = slabs // 2
    half = ny // 2
    win = half + PAD
    other = 1 - h
    partner = s + 1 - 2 * h
    first_row = pl.multiple_of(h * (half - PAD), 8)
    partner_row = pl.multiple_of(other * (half - PAD), 8)
    own = pl.multiple_of(PAD * h, 8)
    mine = pl.multiple_of(h * half, 8)
    has_next = t < slices - 1
    has_prev = t > 0
    has_lower = p > 0
    has_upper = p < pairs - 1
    pending = []

    def start(copy, cond=None):
        if cond is None:
            copy.start()
        else:
            pl.when(cond)(copy.start)
        return copy

    def later(copy, cond=None):
        pending.append((copy, cond))

    def remote(src, dst, send, recv, tm, space):
        return pltpu.make_async_remote_copy(
            src_ref=src, dst_ref=dst, send_sem=send, recv_sem=recv,
            device_id=(tm, space), device_id_type=MESH,
        )

    barrier = pltpu.get_barrier_semaphore()

    def greet(d, carry):
        pl.semaphore_signal(
            barrier, inc=1, device_id=(t, lax.rem(s + d, slabs)), device_id_type=MESH
        )
        return carry

    lax.fori_loop(1, slabs, greet, 0)
    for cond, tm in ((has_next, t + 1), (has_prev, t - 1)):

        @pl.when(cond)
        def _(tm=tm):
            for space in (s, partner):
                pl.semaphore_signal(barrier, inc=1, device_id=(tm, space), device_id_type=MESH)

    sources = [kappa_in.at[0]] + [nodes_in.at[0, j, 0] for j in range(3)] + [start_in.at[0, 0]]
    loads = []
    for k, source in enumerate(sources):
        loads.append(
            start(
                pltpu.make_async_copy(
                    source.at[pl.ds(first_row, win)], field.at[k, h, pl.ds(PAD, win)], own_s.at[k]
                )
            )
        )

    zeros = jnp.zeros((PAD, nz), f32)
    for k in range(FIELDS):
        for slab in range(2):
            field[k, slab, 0:PAD, :] = zeros
            field[k, slab, win + PAD : win + 2 * PAD, :] = zeros

    def clear(ref):
        def body(i, carry):
            for k in range(HALOS):
                ref[k, pl.ds(pl.multiple_of(i * 8, 8), 8), :] = zeros
            return carry

        lax.fori_loop(0, win // 8, body, 0)

    @pl.when(jnp.logical_not(has_lower))
    def _():
        clear(lower)

    @pl.when(jnp.logical_not(has_upper))
    def _():
        clear(upper)

    pl.semaphore_wait(
        barrier,
        slabs - 1 + 2 * has_next.astype(jnp.int32) + 2 * has_prev.astype(jnp.int32),
    )

    chunk = tile_of(win, win // 3)
    chunks = win // chunk

    def swap_copy(k, c):
        return remote(
            sources[k].at[pl.ds(partner_row + c * chunk, chunk)],
            field.at[k, h, pl.ds(PAD + c * chunk, chunk)],
            swap_s.at[k, c], swap_r.at[k, c], t, partner,
        )

    def swap_wait(k, c):
        remote(
            field.at[k, other, pl.ds(PAD + c * chunk, chunk)],
            field.at[k, other, pl.ds(PAD + c * chunk, chunk)],
            swap_s.at[k, c], swap_r.at[k, c], t, partner,
        ).wait_recv()

    for k in range(5):
        for c in range(chunks):
            later(start(swap_copy(k, c)))

    def down(f, k, c, lo, rows):
        return remote(
            field.at[f, 0, pl.ds(PAD + lo, rows)], upper.at[k, pl.ds(lo, rows)],
            halo_s.at[k, 0, c], halo_r.at[k, 0, c], t, s - 2,
        )

    def up(f, k, c, lo, rows):
        return remote(
            field.at[f, 1, pl.ds(PAD + lo, rows)], lower.at[k, pl.ds(lo, rows)],
            halo_s.at[k, 1, c], halo_r.at[k, 1, c], t, s + 2,
        )

    def first_hop(k, c, which):
        @pl.when(jnp.logical_and(which == 0, has_lower))
        def _():
            down(k, k, c, c * chunk, chunk).start()

        @pl.when(jnp.logical_and(which == 1, has_upper))
        def _():
            up(k, k, c, c * chunk, chunk).start()

    for k in range(4):
        loads[k].wait()
        for c in range(chunks):
            first_hop(k, c, h)
    loads[4].wait()

    def pass_on(k):
        for c in range(chunks):
            swap_wait(k, c)
            first_hop(k, c, other)

    def halo_wait(k, c, lo, rows, sides=(0, 1)):
        if 0 in sides:

            @pl.when(has_upper)
            def _():
                remote(
                    upper.at[k, pl.ds(lo, rows)], upper.at[k, pl.ds(lo, rows)],
                    halo_s.at[k, 0, c], halo_r.at[k, 0, c], t, s + 2,
                ).wait_recv()

        if 1 in sides:

            @pl.when(has_lower)
            def _():
                remote(
                    lower.at[k, pl.ds(lo, rows)], lower.at[k, pl.ds(lo, rows)],
                    halo_s.at[k, 1, c], halo_r.at[k, 1, c], t, s - 2,
                ).wait_recv()

    def halo_sent(f, k, c, lo, rows):
        later(down(f, k, c, lo, rows), has_lower)
        later(up(f, k, c, lo, rows), has_upper)

    for k in range(4):
        for c in range(chunks):
            halo_sent(k, k, c, c * chunk, chunk)

    tile = tile_of(win, 24)
    lane = lax.broadcasted_iota(jnp.int32, (tile, nz), 1)

    def loop(rows, size, body, init=0, offset=0):
        def step(i, carry):
            return body(pl.multiple_of(offset + i * size, 8), carry)

        return lax.fori_loop(0, rows // size, step, init)

    def coefficients(b, carry):
        windows = [field[KAPPA, slab, pl.ds(b, tile + 2 * PAD), :] for slab in range(2)]
        centre = [w[PAD : PAD + tile] for w in windows]
        before = 0.5 * (centre[0] + lower[H_KAPPA, pl.ds(b, tile), :])
        between = 0.5 * (centre[0] + centre[1])
        after = 0.5 * (centre[1] + upper[H_KAPPA, pl.ds(b, tile), :])
        across[0, pl.ds(b, tile), :] = before
        across[1, pl.ds(b, tile), :] = between
        across[2, pl.ds(b, tile), :] = after
        ends = [before + between, between + after]
        for slab in range(2):
            w, k = windows[slab], centre[slab]
            above = 0.5 * (k + w[PAD - 1 : PAD - 1 + tile])
            below = 0.5 * (k + w[PAD + 1 : PAD + 1 + tile])
            right = jnp.where(lane == nz - 1, 0.0, pltpu.roll(k, nz - 1, axis=1))
            left = jnp.where(lane == 0, 0.0, pltpu.roll(k, 1, axis=1))
            right_face = 0.5 * (k + right)
            left_face = 0.5 * (k + left)
            faces[0, slab, pl.ds(b, tile), :] = above
            faces[1, slab, pl.ds(b, tile), :] = below
            faces[2, slab, pl.ds(b, tile), :] = jnp.where(lane == nz - 1, 0.0, right_face)
            faces[3, slab, pl.ds(b, tile), :] = ends[slab] + above + below + right_face + left_face
        return carry

    def heat(windows, outer, b, size):
        centre = [w[PAD : PAD + size] for w in windows]
        between = across[1, pl.ds(b, size), :]
        images = []
        for slab in range(2):
            w, v = windows[slab], centre[slab]
            fz = faces[2, slab, pl.ds(b, size), :]
            value = between * centre[1 - slab]
            if outer[slab] is not None:
                value = value + outer[slab]
            value = value + faces[0, slab, pl.ds(b, size), :] * w[PAD - 1 : PAD - 1 + size]
            value = value + faces[1, slab, pl.ds(b, size), :] * w[PAD + 1 : PAD + 1 + size]
            value = value + fz * pltpu.roll(v, nz - 1, axis=1) + pltpu.roll(fz * v, 1, axis=1)
            images.append(value - faces[3, slab, pl.ds(b, size), :] * v)
        return centre, images

    def plain_heat(f, k, b, size):
        windows = [field[f, slab, pl.ds(b, size + 2 * PAD), :] for slab in range(2)]
        outer = (
            across[0, pl.ds(b, size), :] * lower[k, pl.ds(b, size), :],
            across[2, pl.ds(b, size), :] * upper[k, pl.ds(b, size), :],
        )
        return heat(windows, outer, b, size)

    def folded(value):
        return jnp.sum(value.reshape(-1, 8, nz), axis=0)

    def sum_copy(e, d):
        return remote(
            sums.at[e, s], sums.at[e, s], sum_s.at[e, d], sum_r.at[e, d],
            t, lax.rem(s + d, slabs),
        )

    def sum_start(e, parts):
        for row, part in enumerate(parts):
            flat = jnp.sum(part, axis=0, keepdims=True)
            line = flat[:, 0:128]
            for at in range(128, nz, 128):
                line = line + flat[:, at : at + 128]
            sums[e, s, row : row + 1, :] = line

        def body(d, carry):
            sum_copy(e, d).start()
            return carry

        lax.fori_loop(1, slabs, body, 0)

    def sum_wait(e):
        def body(d, carry):
            source = lax.rem(s - d + slabs, slabs)
            remote(
                sums.at[e, source], sums.at[e, source], sum_s.at[e, d], sum_r.at[e, d],
                t, source,
            ).wait_recv()
            return carry

        lax.fori_loop(1, slabs, body, 0)
        total = jnp.sum(sums[e], axis=0)
        total = jnp.sum(total, axis=1, keepdims=True)
        return total[0:1, :], total[1:2, :]

    def res_send(m):
        start(down(RES + m, H_RES + m, 0, 0, win), has_lower)
        start(up(RES + m, H_RES + m, 0, 0, win), has_upper)
        halo_sent(RES + m, H_RES + m, 0, 0, win)

    quarter = half // 2
    set_up = own
    set_down = pl.multiple_of(own + quarter, 8)

    def img_send(m):
        copies = (
            (down(IMG + m, H_IMG + m, 0, set_down, quarter), has_lower),
            (up(IMG + m, H_IMG + m, 0, set_up, quarter), has_upper),
        )
        for copy, cond in copies:
            start(copy, cond)
            later(copy, cond)

    def product(m):
        halo_wait(H_RES + m, 0, 0, win)

        def body(b, carry):
            centre, images = plain_heat(RES + m, H_RES + m, b, tile)
            row = lax.broadcasted_iota(jnp.int32, (tile, nz), 0) + b
            inside = jnp.logical_and(row >= own, row < own + half)
            norm, along = carry
            for slab in range(2):
                v = centre[slab]
                z = v - WIDTHS[m] * images[slab]
                field[IMG + m, slab, pl.ds(PAD + b, tile), :] = z
                masked = jnp.where(inside, v, 0.0)
                norm = norm + folded(masked * v)
                along = along + folded(masked * z)
            return norm, along

        nothing = jnp.zeros((8, nz), f32)
        norm, along = loop(win, tile, body, (nothing, nothing))
        img_send(m)
        sum_start(2 * m, (norm, along))

    small = tile_of(quarter, 32)

    def second(m):
        norm_now, along = sum_wait(2 * m)
        step_size = norm_now / along
        halo_wait(H_IMG + m, 0, set_down, quarter, (0,))
        halo_wait(H_IMG + m, 0, set_up, quarter, (1,))

        def body_of(side):
            ref = lower if side == 0 else upper

            def body(b, carry):
                windows = [
                    field[RES + m, slab, pl.ds(b, small + 2 * PAD), :]
                    - step_size * field[IMG + m, slab, pl.ds(b, small + 2 * PAD), :]
                    for slab in range(2)
                ]
                beside = (
                    ref[H_RES + m, pl.ds(b, small), :]
                    - step_size * ref[H_IMG + m, pl.ds(b, small), :]
                )
                term = 2.0 * across[2 * side, pl.ds(b, small), :] * beside
                outer = (term, None) if side == 0 else (None, term)
                centre, images = heat(windows, outer, b, small)
                norm, along = carry
                for slab in range(2):
                    v = centre[slab]
                    norm = norm + folded(v * v)
                    along = along + folded(v * (v - WIDTHS[m] * images[slab]))
                return norm, along

            return body

        nothing = jnp.zeros((8, nz), f32)
        carry = loop(quarter, small, body_of(0), (nothing, nothing), set_up)
        carry = loop(quarter, small, body_of(1), carry, set_down)
        sum_start(2 * m + 1, carry)
        return norm_now, step_size

    def factors(m, norm_now, step_size):
        norm_next, along = sum_wait(2 * m + 1)
        momentum = norm_next / norm_now
        step_next = norm_next / (along - momentum * norm_next / step_size)
        return step_size + step_next * (1.0 + momentum), step_size * step_next

    def finish(m, scalars):
        on_res, on_img = factors(m, *scalars)
        node = NODE + min(m, 2)

        def body(b, carry):
            at = pl.ds(PAD + b, tile)
            for slab in range(2):
                x = (
                    field[node, slab, at, :]
                    + on_res * field[RES + m, slab, at, :]
                    - on_img * field[IMG + m, slab, at, :]
                )
                result[m, slab, pl.ds(b, tile), :] = x
                if m < 2:
                    field[RES + m + 1, slab, at, :] = x + base[m, slab, pl.ds(b, tile), :]
            return carry

        loop(win, tile, body)

    def old_image(j):
        for c in range(chunks):
            halo_wait(H_NODE + j, c, c * chunk, chunk)

        def body(b, carry):
            _, images = plain_heat(NODE + j, H_NODE + j, b, tile)
            for slab in range(2):
                image[j, slab, pl.ds(b, tile), :] = images[slab]
            return carry

        loop(win, tile, body)

    pass_on(KAPPA)
    pass_on(NODE)
    for c in range(chunks):
        halo_wait(H_KAPPA, c, c * chunk, chunk)
    loop(win, tile, coefficients)
    pass_on(NODE + 1)
    old_image(0)
    pass_on(NODE + 2)
    old_image(1)
    for c in range(chunks):
        swap_wait(START, c)
    for c in range(chunks):
        halo_wait(H_NODE + 2, c, c * chunk, chunk)

    def residuals(b, carry):
        _, last = plain_heat(NODE + 2, H_NODE + 2, b, tile)
        at = pl.ds(PAD + b, tile)
        for slab in range(2):
            images = [image[0, slab, pl.ds(b, tile), :], image[1, slab, pl.ds(b, tile), :], last[slab]]
            begin = field[START, slab, at, :]
            parts = []
            for row in range(4):
                weights = COLLOC[2] if row == 3 else [sweep_weight(row, j) for j in range(3)]
                value = (STEP * weights[0]) * images[0]
                for j in range(1, 3):
                    value = value + (STEP * weights[j]) * images[j]
                parts.append(value - field[NODE + min(row, 2), slab, at, :])
            field[RES, slab, at, :] = begin + parts[0]
            base[0, slab, pl.ds(b, tile), :] = parts[1]
            base[1, slab, pl.ds(b, tile), :] = parts[2]
            field[RES + 3, slab, at, :] = begin + parts[3]
        return carry

    loop(win, tile, residuals)

    def give_back(m):
        later(
            start(
                remote(
                    result.at[m, other, pl.ds(own, half)], fine_out.at[0, m, 0, pl.ds(mine, half)],
                    out_s.at[m], out_r.at[m], t, partner,
                )
            )
        )
        keep = pltpu.make_async_copy(
            result.at[m, h, pl.ds(own, half)], fine_out.at[0, m, 0, pl.ds(mine, half)], keep_s.at[m]
        )
        keep.start()
        return keep

    theirs = pl.multiple_of(other * half, 8)

    @pl.when(jnp.logical_not(has_prev))
    def _():
        pltpu.make_async_copy(start_in.at[0, 0], staged, copy_s.at[0]).start()

    res_send(0)
    product(0)
    res_send(3)
    scalars = second(0)
    finish(0, scalars)
    res_send(1)
    keeps = [give_back(0)]
    product(3)
    product(1)
    scalars = second(1)
    scalars_coarse = second(3)
    finish(1, scalars)
    res_send(2)
    keeps.append(give_back(1))
    finish(3, scalars_coarse)

    def coarse_copies():
        return [
            remote(
                result.at[3, h, pl.ds(own, half)], coarse_out.at[0, 0, pl.ds(mine, half)],
                end_s.at[0], end_r.at[0], t + 1, s,
            ),
            remote(
                result.at[3, other, pl.ds(own, half)], coarse_out.at[0, 0, pl.ds(mine, half)],
                end_s.at[1], end_r.at[1], t + 1, partner,
            ),
        ]

    for copy in coarse_copies():
        start(copy, has_next)
        later(copy, has_next)

    @pl.when(jnp.logical_not(has_prev))
    def _():
        pltpu.make_async_copy(start_in.at[0, 0], staged, copy_s.at[0]).wait()
        first = pltpu.make_async_copy(staged, start_out.at[0, 0], copy_s.at[0])
        second_copy = pltpu.make_async_copy(staged, coarse_out.at[0, 0], copy_s.at[1])
        first.start()
        second_copy.start()
        first.wait()
        second_copy.wait()

    product(2)
    scalars = second(2)
    finish(2, scalars)

    pieces = 2
    piece = half // pieces
    for c in range(pieces):
        later(
            start(
                remote(
                    result.at[2, other, pl.ds(own + c * piece, piece)],
                    mail.at[pl.ds(c * piece, piece)],
                    out_s.at[2 + c], out_r.at[2 + c], t, partner,
                )
            )
        )
    for c in range(pieces):
        rows = pl.ds(mine + c * piece, piece)
        src = result.at[2, h, pl.ds(own + c * piece, piece)]
        copy = remote(src, start_out.at[0, 0, rows], end_s.at[2 + c], end_r.at[2 + c], t + 1, s)
        start(copy, has_next)
        later(copy, has_next)
        keep = pltpu.make_async_copy(src, fine_out.at[0, 2, 0, rows], keep_s.at[2 + c])
        keep.start()
        keeps.append(keep)
    for c in range(pieces):
        rows = pl.ds(theirs + c * piece, piece)
        src = mail.at[pl.ds(c * piece, piece)]
        remote(src, src, out_s.at[2 + c], out_r.at[2 + c], t, partner).wait_recv()
        copy = remote(
            src, start_out.at[0, 0, rows],
            end_s.at[2 + pieces + c], end_r.at[2 + pieces + c], t + 1, s,
        )
        start(copy, has_next)
        later(copy, has_next)
        keep = pltpu.make_async_copy(src, fine_out.at[0, 2, 0, rows], keep_s.at[2 + pieces + c])
        keep.start()
        keeps.append(keep)

    for m in range(2):
        dst = fine_out.at[0, m, 0, pl.ds(theirs, half)]
        remote(dst, dst, out_s.at[m], out_r.at[m], t, partner).wait_recv()

    @pl.when(has_prev)
    def _():
        for k in range(2):
            at = mine if k == 0 else theirs
            dst = coarse_out.at[0, 0, pl.ds(at, half)]
            remote(dst, dst, end_s.at[k], end_r.at[k], t - 1, s).wait_recv()
        for k in range(2):
            at = mine if k == 0 else theirs
            for c in range(pieces):
                dst = start_out.at[0, 0, pl.ds(at + c * piece, piece)]
                e = 2 + k * pieces + c
                remote(dst, dst, end_s.at[e], end_r.at[e], t - 1, s).wait_recv()

    for keep in keeps:
        keep.wait()
    for copy, cond in pending:
        if cond is None:
            copy.wait_send()
        else:
            pl.when(cond)(copy.wait_send)

    def drain(d, carry):
        for e in range(8):
            sum_copy(e, d).wait_send()
        return carry

    lax.fori_loop(1, slabs, drain, 0)


def solution(mesh):
    slices, slabs = mesh.shape["tm"], mesh.shape["space"]

    def on_device(start_value, old_nodes, diffusivity):
        ny, nz = start_value.shape[2:]
        half = ny // 2
        win = half + PAD
        chunks = win // tile_of(win, win // 3)
        vmem = lambda *shape: pltpu.VMEM(shape, jnp.float32)
        dma = lambda *shape: pltpu.SemaphoreType.DMA(shape)

        def body(*refs):
            kernel(slices, slabs, ny, nz, *refs)

        return pl.pallas_call(
            body,
            out_shape=(
                jax.ShapeDtypeStruct(old_nodes.shape, jnp.float32),
                jax.ShapeDtypeStruct(start_value.shape, jnp.float32),
                jax.ShapeDtypeStruct(start_value.shape, jnp.float32),
            ),
            in_specs=[pl.BlockSpec(memory_space=pl.ANY)] * 3,
            out_specs=(pl.BlockSpec(memory_space=pl.ANY),) * 3,
            scratch_shapes=[
                vmem(FIELDS, 2, win + 2 * PAD, nz),
                vmem(HALOS, win, nz),
                vmem(HALOS, win, nz),
                vmem(4, 2, win, nz),
                vmem(3, win, nz),
                vmem(2, 2, win, nz),
                vmem(2, 2, win, nz),
                vmem(4, 2, win, nz),
                vmem(ny, nz),
                vmem(half, nz),
                vmem(8, slabs, 2, 128),
                dma(5, chunks), dma(5, chunks), dma(5),
                dma(HALOS, 2, chunks), dma(HALOS, 2, chunks),
                dma(8, slabs), dma(8, slabs),
                dma(4), dma(4), dma(6), dma(6), dma(6), dma(2),
            ],
            compiler_params=pltpu.CompilerParams(
                collective_id=0, has_side_effects=True, vmem_limit_bytes=60 * 1024 * 1024
            ),
            name="pfasst",
        )(start_value, old_nodes, diffusivity)

    in_specs = (
        P("tm", "space", None, None),
        P("tm", None, "space", None, None),
        P("space", None, None),
    )
    out_specs = (
        P("tm", None, "space", None, None),
        P("tm", "space", None, None),
        P("tm", "space", None, None),
    )
    return jax.shard_map(
        on_device, mesh=mesh, in_specs=in_specs, out_specs=out_specs, check_vma=False
    )
```

```python
import math

import jax
import jax.numpy as jnp
from jax import lax
from jax.experimental import pallas as pl
from jax.experimental.pallas import tpu as pltpu
from jax.sharding import PartitionSpec as P

STEP = 2.0
ROOT_SIX = math.sqrt(6.0)
NODE_TIMES = [(4.0 - ROOT_SIX) / 10.0, (4.0 + ROOT_SIX) / 10.0, 1.0]
COLLOC = [
    [
        (88.0 - 7.0 * ROOT_SIX) / 360.0,
        (296.0 - 169.0 * ROOT_SIX) / 1800.0,
        (-2.0 + 3.0 * ROOT_SIX) / 225.0,
    ],
    [
        (296.0 + 169.0 * ROOT_SIX) / 1800.0,
        (88.0 + 7.0 * ROOT_SIX) / 360.0,
        (-2.0 - 3.0 * ROOT_SIX) / 225.0,
    ],
    [(16.0 - ROOT_SIX) / 36.0, (16.0 + ROOT_SIX) / 36.0, 1.0 / 9.0],
]
MESH = pl.DeviceIdType.MESH
PAD = 8

KAPPA, NODE, START, RES, IMG, GAIN = 0, 1, 4, 5, 9, 13
FIELDS = 15
H_KAPPA, H_NODE, H_RES, H_IMG, H_GAIN = 0, 1, 4, 8, 12
HALOS = 14


def sweep_weight(row, column):
    below = COLLOC[row - 1][column] if row > 0 else 0.0
    return COLLOC[row][column] - below


def node_width(row):
    below = NODE_TIMES[row - 1] if row > 0 else 0.0
    return NODE_TIMES[row] - below


WIDTHS = [STEP * node_width(0), STEP * node_width(1), STEP * node_width(2), STEP]


def chunk_bounds(rows, tile):
    tiles = rows // tile
    parts = min(3, tiles)
    cuts = [tile * (-(-tiles * c // parts)) for c in range(parts + 1)]
    return [(cuts[c], cuts[c + 1] - cuts[c]) for c in range(parts)]


def tile_of(rows, most):
    best = 8
    for size in range(8, most + 1, 8):
        if rows % size == 0:
            best = size
    return best


def kernel(
    slices, slabs, ny, nz,
    start_in, nodes_in, kappa_in,
    fine_out, start_out, coarse_out,
    field, lower, upper, faces, across, result, staged, mail, sums,
    swap_s, swap_r, own_s, halo_s, halo_r, sum_s, sum_r, out_s, out_r, keep_s, end_s, end_r, copy_s,
):
    f32 = jnp.float32
    t = lax.axis_index("tm")
    s = lax.axis_index("space")
    h = lax.rem(s, 2)
    p = lax.div(s, 2)
    pairs = slabs // 2
    half = ny // 2
    win = half + PAD
    other = 1 - h
    partner = s + 1 - 2 * h
    first_row = pl.multiple_of(h * (half - PAD), 8)
    partner_row = pl.multiple_of(other * (half - PAD), 8)
    own = pl.multiple_of(PAD * h, 8)
    mine = pl.multiple_of(h * half, 8)
    has_next = t < slices - 1
    has_prev = t > 0
    has_lower = p > 0
    has_upper = p < pairs - 1
    pending = []

    def start(copy, cond=None):
        if cond is None:
            copy.start()
        else:
            pl.when(cond)(copy.start)
        return copy

    def later(copy, cond=None):
        pending.append((copy, cond))

    def remote(src, dst, send, recv, tm, space):
        return pltpu.make_async_remote_copy(
            src_ref=src, dst_ref=dst, send_sem=send, recv_sem=recv,
            device_id=(tm, space), device_id_type=MESH,
        )

    barrier = pltpu.get_barrier_semaphore()

    def greet(d, carry):
        pl.semaphore_signal(
            barrier, inc=1, device_id=(t, lax.rem(s + d, slabs)), device_id_type=MESH
        )
        return carry

    lax.fori_loop(1, slabs, greet, 0)
    for cond, tm in ((has_next, t + 1), (has_prev, t - 1)):

        @pl.when(cond)
        def _(tm=tm):
            for space in (s, partner):
                pl.semaphore_signal(barrier, inc=1, device_id=(tm, space), device_id_type=MESH)

    sources = [kappa_in.at[0]] + [nodes_in.at[0, j, 0] for j in range(3)] + [start_in.at[0, 0]]
    loads = []
    for k, source in enumerate(sources):
        loads.append(
            start(
                pltpu.make_async_copy(
                    source.at[pl.ds(first_row, win)], field.at[k, h, pl.ds(PAD, win)], own_s.at[k]
                )
            )
        )

    zeros = jnp.zeros((PAD, nz), f32)
    for k in range(FIELDS):
        for slab in range(2):
            field[k, slab, 0:PAD, :] = zeros
            field[k, slab, win + PAD : win + 2 * PAD, :] = zeros

    def clear(ref):
        def body(i, carry):
            for k in range(HALOS):
                ref[k, pl.ds(pl.multiple_of(i * 8, 8), 8), :] = zeros
            return carry

        lax.fori_loop(0, win // 8, body, 0)

    @pl.when(jnp.logical_not(has_lower))
    def _():
        clear(lower)

    @pl.when(jnp.logical_not(has_upper))
    def _():
        clear(upper)

    pl.semaphore_wait(
        barrier,
        slabs - 1 + 2 * has_next.astype(jnp.int32) + 2 * has_prev.astype(jnp.int32),
    )

    tile = tile_of(win, 24)
    bounds = chunk_bounds(win, tile)
    chunks = len(bounds)

    def swap_copy(k, c):
        lo, rows = bounds[c]
        return remote(
            sources[k].at[pl.ds(partner_row + lo, rows)],
            field.at[k, h, pl.ds(PAD + lo, rows)],
            swap_s.at[k, c], swap_r.at[k, c], t, partner,
        )

    def swap_wait(k, c):
        lo, rows = bounds[c]
        dst = field.at[k, other, pl.ds(PAD + lo, rows)]
        remote(dst, dst, swap_s.at[k, c], swap_r.at[k, c], t, partner).wait_recv()

    for c in range(chunks):
        for k in range(5):
            later(start(swap_copy(k, c)))

    def down(f, k, c, lo, rows):
        return remote(
            field.at[f, 0, pl.ds(PAD + lo, rows)], upper.at[k, pl.ds(lo, rows)],
            halo_s.at[k, 0, c], halo_r.at[k, 0, c], t, s - 2,
        )

    def up(f, k, c, lo, rows):
        return remote(
            field.at[f, 1, pl.ds(PAD + lo, rows)], lower.at[k, pl.ds(lo, rows)],
            halo_s.at[k, 1, c], halo_r.at[k, 1, c], t, s + 2,
        )

    def first_hop(k, c, which):
        @pl.when(jnp.logical_and(which == 0, has_lower))
        def _():
            down(k, k, c, *bounds[c]).start()

        @pl.when(jnp.logical_and(which == 1, has_upper))
        def _():
            up(k, k, c, *bounds[c]).start()

    for copy in loads:
        copy.wait()
    for c in range(chunks):
        for k in range(4):
            first_hop(k, c, h)

    def halo_wait(k, c, lo, rows, sides=(0, 1)):
        if 0 in sides:

            @pl.when(has_upper)
            def _():
                remote(
                    upper.at[k, pl.ds(lo, rows)], upper.at[k, pl.ds(lo, rows)],
                    halo_s.at[k, 0, c], halo_r.at[k, 0, c], t, s + 2,
                ).wait_recv()

        if 1 in sides:

            @pl.when(has_lower)
            def _():
                remote(
                    lower.at[k, pl.ds(lo, rows)], lower.at[k, pl.ds(lo, rows)],
                    halo_s.at[k, 1, c], halo_r.at[k, 1, c], t, s - 2,
                ).wait_recv()

    def halo_sent(f, k, c, lo, rows):
        later(down(f, k, c, lo, rows), has_lower)
        later(up(f, k, c, lo, rows), has_upper)

    for k in range(4):
        for c in range(chunks):
            halo_sent(k, k, c, *bounds[c])

    lane = lax.broadcasted_iota(jnp.int32, (tile, nz), 1)

    def loop(rows, size, body, init=0, offset=0):
        def step(i, carry):
            return body(pl.multiple_of(offset + i * size, 8), carry)

        return lax.fori_loop(0, rows // size, step, init)

    def coefficients(b, carry):
        windows = [field[KAPPA, slab, pl.ds(b, tile + 2 * PAD), :] for slab in range(2)]
        centre = [w[PAD : PAD + tile] for w in windows]
        before = 0.5 * (centre[0] + lower[H_KAPPA, pl.ds(b, tile), :])
        between = 0.5 * (centre[0] + centre[1])
        after = 0.5 * (centre[1] + upper[H_KAPPA, pl.ds(b, tile), :])
        across[0, pl.ds(b, tile), :] = before
        across[1, pl.ds(b, tile), :] = between
        across[2, pl.ds(b, tile), :] = after
        ends = [before + between, between + after]
        for slab in range(2):
            w, k = windows[slab], centre[slab]
            above = 0.5 * (k + w[PAD - 1 : PAD - 1 + tile])
            below = 0.5 * (k + w[PAD + 1 : PAD + 1 + tile])
            right = jnp.where(lane == nz - 1, 0.0, pltpu.roll(k, nz - 1, axis=1))
            left = jnp.where(lane == 0, 0.0, pltpu.roll(k, 1, axis=1))
            right_face = 0.5 * (k + right)
            left_face = 0.5 * (k + left)
            faces[0, slab, pl.ds(b, tile), :] = above
            faces[1, slab, pl.ds(b, tile), :] = below
            faces[2, slab, pl.ds(b, tile), :] = jnp.where(lane == nz - 1, 0.0, right_face)
            faces[3, slab, pl.ds(b, tile), :] = ends[slab] + above + below + right_face + left_face
        return carry

    def heat(windows, outer, b, size):
        centre = [w[PAD : PAD + size] for w in windows]
        between = across[1, pl.ds(b, size), :]
        images = []
        for slab in range(2):
            w, v = windows[slab], centre[slab]
            fz = faces[2, slab, pl.ds(b, size), :]
            value = between * centre[1 - slab]
            if outer[slab] is not None:
                value = value + outer[slab]
            value = value + faces[0, slab, pl.ds(b, size), :] * w[PAD - 1 : PAD - 1 + size]
            value = value + faces[1, slab, pl.ds(b, size), :] * w[PAD + 1 : PAD + 1 + size]
            value = value + fz * pltpu.roll(v, nz - 1, axis=1) + pltpu.roll(fz * v, 1, axis=1)
            images.append(value - faces[3, slab, pl.ds(b, size), :] * v)
        return centre, images

    def plain_heat(f, k, b, size):
        windows = [field[f, slab, pl.ds(b, size + 2 * PAD), :] for slab in range(2)]
        outer = (
            across[0, pl.ds(b, size), :] * lower[k, pl.ds(b, size), :],
            across[2, pl.ds(b, size), :] * upper[k, pl.ds(b, size), :],
        )
        return heat(windows, outer, b, size)

    def folded(value):
        return jnp.sum(value.reshape(-1, 8, nz), axis=0)

    def sum_copy(e, d):
        return remote(
            sums.at[e, s], sums.at[e, s], sum_s.at[e, d], sum_r.at[e, d],
            t, lax.rem(s + d, slabs),
        )

    def sum_start(e, parts):
        for row, part in enumerate(parts):
            flat = jnp.sum(part, axis=0, keepdims=True)
            line = flat[:, 0:128]
            for at in range(128, nz, 128):
                line = line + flat[:, at : at + 128]
            sums[e, s, row : row + 1, :] = line

        def body(d, carry):
            sum_copy(e, d).start()
            return carry

        lax.fori_loop(1, slabs, body, 0)

    def sum_wait(e):
        def body(d, carry):
            source = lax.rem(s - d + slabs, slabs)
            remote(
                sums.at[e, source], sums.at[e, source], sum_s.at[e, d], sum_r.at[e, d],
                t, source,
            ).wait_recv()
            return carry

        lax.fori_loop(1, slabs, body, 0)
        total = jnp.sum(sums[e], axis=0)
        total = jnp.sum(total, axis=1, keepdims=True)
        return total[0:1, :], total[1:2, :]

    def halo_send(f, k, c, lo, rows):
        start(down(f, k, c, lo, rows), has_lower)
        start(up(f, k, c, lo, rows), has_upper)
        halo_sent(f, k, c, lo, rows)

    quarter = half // 2
    set_up = own
    set_down = pl.multiple_of(own + quarter, 8)
    pieces_of = (
        ((quarter, quarter + PAD), (0, quarter + PAD)),
        ((0, quarter), (quarter + PAD, quarter)),
    )

    def img_send(m, piece):
        (lo_d, rows_d), (lo_u, rows_u) = pieces_of[piece]
        copies = (
            (down(IMG + m, H_IMG + m, piece, lo_d, rows_d), has_lower),
            (up(IMG + m, H_IMG + m, piece, lo_u, rows_u), has_upper),
        )
        for copy, cond in copies:
            start(copy, cond)
            later(copy, cond)

    def img_wait(m, piece):
        halo_wait(H_IMG + m, piece, *pieces_of[piece][0], (0,))
        halo_wait(H_IMG + m, piece, *pieces_of[piece][1], (1,))

    def product(m):
        def body(b, carry):
            centre, images = plain_heat(RES + m, H_RES + m, b, tile)
            row = lax.broadcasted_iota(jnp.int32, (tile, nz), 0) + b
            inside = jnp.logical_and(row >= own, row < own + half)
            norm, along = carry
            for slab in range(2):
                v = centre[slab]
                z = v - WIDTHS[m] * images[slab]
                field[IMG + m, slab, pl.ds(PAD + b, tile), :] = z
                masked = jnp.where(inside, v, 0.0)
                norm = norm + folded(masked * v)
                along = along + folded(masked * z)
            return norm, along

        nothing = jnp.zeros((8, nz), f32)
        norm, along = loop(win, tile, body, (nothing, nothing))
        sum_start(2 * m, (norm, along))
        img_send(m, 0)

    small = tile_of(quarter, 32)

    def second(m):
        norm_now, along = sum_wait(2 * m)
        step_size = norm_now / along
        img_wait(m, 0)

        def body_of(side):
            ref = lower if side == 0 else upper

            def body(b, carry):
                windows = [
                    field[RES + m, slab, pl.ds(b, small + 2 * PAD), :]
                    - step_size * field[IMG + m, slab, pl.ds(b, small + 2 * PAD), :]
                    for slab in range(2)
                ]
                beside = (
                    ref[H_RES + m, pl.ds(b, small), :]
                    - step_size * ref[H_IMG + m, pl.ds(b, small), :]
                )
                term = 2.0 * across[2 * side, pl.ds(b, small), :] * beside
                outer = (term, None) if side == 0 else (None, term)
                centre, images = heat(windows, outer, b, small)
                norm, along = carry
                for slab in range(2):
                    v = centre[slab]
                    norm = norm + folded(v * v)
                    along = along + folded(v * (v - WIDTHS[m] * images[slab]))
                return norm, along

            return body

        nothing = jnp.zeros((8, nz), f32)
        carry = loop(quarter, small, body_of(0), (nothing, nothing), set_up)
        carry = loop(quarter, small, body_of(1), carry, set_down)
        sum_start(2 * m + 1, carry)
        return norm_now, step_size

    def factors(m, norm_now, step_size):
        norm_next, along = sum_wait(2 * m + 1)
        momentum = norm_next / norm_now
        step_next = norm_next / (along - momentum * norm_next / step_size)
        return step_size + step_next * (1.0 + momentum), step_size * step_next

    def advance(m, scalars):
        on_res, on_img = scalars
        for c in range(chunks):
            halo_wait(H_GAIN + m, c, *spans[c])
        img_wait(m, 1)

        def body(b, carry):
            at = pl.ds(PAD + b, tile)
            rows = pl.ds(b, tile)
            for slab in range(2):
                field[RES + m + 1, slab, at, :] = (
                    field[GAIN + m, slab, at, :]
                    + on_res * field[RES + m, slab, at, :]
                    - on_img * field[IMG + m, slab, at, :]
                )
            for ref in (lower, upper):
                ref[H_RES + m + 1, rows, :] = (
                    ref[H_GAIN + m, rows, :]
                    + on_res * ref[H_RES + m, rows, :]
                    - on_img * ref[H_IMG + m, rows, :]
                )
            return carry

        loop(win, tile, body)

    def coarse_residual():
        def body(b, carry):
            at = pl.ds(PAD + b, tile)
            rows = pl.ds(b, tile)
            for slab in range(2):
                field[RES + 3, slab, at, :] = (
                    field[RES, slab, at, :] + field[GAIN, slab, at, :] + field[GAIN + 1, slab, at, :]
                )
            for ref in (lower, upper):
                ref[H_RES + 3, rows, :] = (
                    ref[H_RES, rows, :] + ref[H_GAIN, rows, :] + ref[H_GAIN + 1, rows, :]
                )
            return carry

        loop(win, tile, body)

    def finish(m, scalars):
        on_res, on_img = scalars
        node = NODE + min(m, 2)

        def body(b, carry):
            for slab in range(2):
                at = pl.ds(PAD + b, small)
                result[m, slab, pl.ds(b, small), :] = (
                    field[node, slab, at, :]
                    + on_res * field[RES + m, slab, at, :]
                    - on_img * field[IMG + m, slab, at, :]
                )
            return carry

        loop(half, small, body, 0, own)

    def residuals(b, carry):
        images = [plain_heat(NODE + j, H_NODE + j, b, tile)[1] for j in range(3)]
        at = pl.ds(PAD + b, tile)
        for slab in range(2):
            nodes = [field[NODE + j, slab, at, :] for j in range(3)]
            ahead = [field[START, slab, at, :]] + nodes
            for row, f in enumerate((RES, GAIN, GAIN + 1)):
                value = ahead[row] - nodes[row]
                for j in range(3):
                    value = value + (STEP * sweep_weight(row, j)) * images[j][slab]
                field[f, slab, at, :] = value
        return carry

    spans = []
    for c, (lo, rows) in enumerate(bounds):
        begin = lo - tile if c else 0
        end = lo + rows - (tile if c < chunks - 1 else 0)
        spans.append((begin, end - begin))

    def begin_rows(c):
        for k in range(4):
            halo_wait(k, c, *bounds[c])
        lo, rows = spans[c]
        loop(rows, tile, coefficients, 0, lo)
        loop(rows, tile, residuals, 0, lo)
        halo_send(RES, H_RES, c, lo, rows)
        if c == 0:
            halo_send(GAIN, H_GAIN, c, lo, rows)

    order = [(k, c) for c in range(chunks) for k in range(5)]
    ready = {}
    for c in range(chunks):
        ready[min(5 * c + 6, len(order) - 1)] = c
    for n, (k, c) in enumerate(order):
        swap_wait(k, c)
        if k < 4:
            first_hop(k, c, other)
        if n in ready:
            begin_rows(ready[n])
    for c in range(1, chunks - 1):
        halo_send(GAIN, H_GAIN, c, *spans[c])

    def give_back(m):
        later(
            start(
                remote(
                    result.at[m, other, pl.ds(own, half)], fine_out.at[0, m, 0, pl.ds(mine, half)],
                    out_s.at[m], out_r.at[m], t, partner,
                )
            )
        )
        keep = pltpu.make_async_copy(
            result.at[m, h, pl.ds(own, half)], fine_out.at[0, m, 0, pl.ds(mine, half)], keep_s.at[m]
        )
        keep.start()
        return keep

    theirs = pl.multiple_of(other * half, 8)

    @pl.when(jnp.logical_not(has_prev))
    def _():
        pltpu.make_async_copy(start_in.at[0, 0], staged, copy_s.at[0]).start()

    for c in range(chunks):
        halo_wait(H_RES, c, *spans[c])
    product(0)
    halo_send(GAIN, H_GAIN, chunks - 1, *spans[chunks - 1])
    scalars = second(0)
    img_send(0, 1)
    halo_send(GAIN + 1, H_GAIN + 1, 0, *spans[0])
    update = factors(0, *scalars)
    advance(0, update)
    product(1)
    for c in range(1, chunks - 1):
        halo_send(GAIN + 1, H_GAIN + 1, c, *spans[c])
    finish(0, update)
    keeps = [give_back(0)]
    @pl.when(jnp.logical_not(has_prev))
    def _():
        pltpu.make_async_copy(start_in.at[0, 0], staged, copy_s.at[0]).wait()
        first = pltpu.make_async_copy(staged, start_out.at[0, 0], copy_s.at[0])
        second_copy = pltpu.make_async_copy(staged, coarse_out.at[0, 0], copy_s.at[1])
        first.start()
        second_copy.start()
        first.wait()
        second_copy.wait()

    scalars = second(1)
    img_send(1, 1)
    halo_send(GAIN + 1, H_GAIN + 1, chunks - 1, *spans[chunks - 1])
    update = factors(1, *scalars)
    advance(1, update)
    product(2)
    coarse_residual()
    product(3)
    scalars = second(2)
    finish(1, update)
    keeps.append(give_back(1))
    scalars_coarse = second(3)
    finish(2, factors(2, *scalars))
    pieces = 2
    piece = half // pieces
    for c in range(pieces):
        later(
            start(
                remote(
                    result.at[2, other, pl.ds(own + c * piece, piece)],
                    mail.at[pl.ds(c * piece, piece)],
                    out_s.at[2 + c], out_r.at[2 + c], t, partner,
                )
            )
        )
    for c in range(pieces):
        rows = pl.ds(mine + c * piece, piece)
        src = result.at[2, h, pl.ds(own + c * piece, piece)]
        copy = remote(src, start_out.at[0, 0, rows], end_s.at[2 + c], end_r.at[2 + c], t + 1, s)
        start(copy, has_next)
        later(copy, has_next)
        keep = pltpu.make_async_copy(src, fine_out.at[0, 2, 0, rows], keep_s.at[2 + c])
        keep.start()
        keeps.append(keep)
    finish(3, factors(3, *scalars_coarse))

    def coarse_copies():
        return [
            remote(
                result.at[3, h, pl.ds(own, half)], coarse_out.at[0, 0, pl.ds(mine, half)],
                end_s.at[0], end_r.at[0], t + 1, s,
            ),
            remote(
                result.at[3, other, pl.ds(own, half)], coarse_out.at[0, 0, pl.ds(mine, half)],
                end_s.at[1], end_r.at[1], t + 1, partner,
            ),
        ]

    for copy in coarse_copies():
        start(copy, has_next)
        later(copy, has_next)

    for c in range(pieces):
        rows = pl.ds(theirs + c * piece, piece)
        src = mail.at[pl.ds(c * piece, piece)]
        remote(src, src, out_s.at[2 + c], out_r.at[2 + c], t, partner).wait_recv()
        copy = remote(
            src, start_out.at[0, 0, rows],
            end_s.at[2 + pieces + c], end_r.at[2 + pieces + c], t + 1, s,
        )
        start(copy, has_next)
        later(copy, has_next)
        keep = pltpu.make_async_copy(src, fine_out.at[0, 2, 0, rows], keep_s.at[2 + pieces + c])
        keep.start()
        keeps.append(keep)

    for m in range(2):
        dst = fine_out.at[0, m, 0, pl.ds(theirs, half)]
        remote(dst, dst, out_s.at[m], out_r.at[m], t, partner).wait_recv()

    @pl.when(has_prev)
    def _():
        for k in range(2):
            at = mine if k == 0 else theirs
            dst = coarse_out.at[0, 0, pl.ds(at, half)]
            remote(dst, dst, end_s.at[k], end_r.at[k], t - 1, s).wait_recv()
        for k in range(2):
            at = mine if k == 0 else theirs
            for c in range(pieces):
                dst = start_out.at[0, 0, pl.ds(at + c * piece, piece)]
                e = 2 + k * pieces + c
                remote(dst, dst, end_s.at[e], end_r.at[e], t - 1, s).wait_recv()

    for keep in keeps:
        keep.wait()
    for copy, cond in pending:
        if cond is None:
            copy.wait_send()
        else:
            pl.when(cond)(copy.wait_send)

    def drain(d, carry):
        for e in range(8):
            sum_copy(e, d).wait_send()
        return carry

    lax.fori_loop(1, slabs, drain, 0)


def solution(mesh):
    slices, slabs = mesh.shape["tm"], mesh.shape["space"]

    def on_device(start_value, old_nodes, diffusivity):
        ny, nz = start_value.shape[2:]
        half = ny // 2
        win = half + PAD
        chunks = len(chunk_bounds(win, tile_of(win, 24)))
        vmem = lambda *shape: pltpu.VMEM(shape, jnp.float32)
        dma = lambda *shape: pltpu.SemaphoreType.DMA(shape)

        def body(*refs):
            kernel(slices, slabs, ny, nz, *refs)

        return pl.pallas_call(
            body,
            out_shape=(
                jax.ShapeDtypeStruct(old_nodes.shape, jnp.float32),
                jax.ShapeDtypeStruct(start_value.shape, jnp.float32),
                jax.ShapeDtypeStruct(start_value.shape, jnp.float32),
            ),
            in_specs=[pl.BlockSpec(memory_space=pl.ANY)] * 3,
            out_specs=(pl.BlockSpec(memory_space=pl.ANY),) * 3,
            scratch_shapes=[
                vmem(FIELDS, 2, win + 2 * PAD, nz),
                vmem(HALOS, win, nz),
                vmem(HALOS, win, nz),
                vmem(4, 2, win, nz),
                vmem(3, win, nz),
                vmem(4, 2, win, nz),
                vmem(ny, nz),
                vmem(half, nz),
                vmem(8, slabs, 2, 128),
                dma(5, chunks), dma(5, chunks), dma(5),
                dma(HALOS, 2, chunks), dma(HALOS, 2, chunks),
                dma(8, slabs), dma(8, slabs),
                dma(4), dma(4), dma(6), dma(6), dma(6), dma(2),
            ],
            compiler_params=pltpu.CompilerParams(
                collective_id=0, has_side_effects=True, vmem_limit_bytes=60 * 1024 * 1024
            ),
            name="pfasst",
        )(start_value, old_nodes, diffusivity)

    in_specs = (
        P("tm", "space", None, None),
        P("tm", None, "space", None, None),
        P("space", None, None),
    )
    out_specs = (
        P("tm", None, "space", None, None),
        P("tm", "space", None, None),
        P("tm", "space", None, None),
    )
    return jax.shard_map(
        on_device, mesh=mesh, in_specs=in_specs, out_specs=out_specs, check_vma=False
    )
```

```python
import math

import jax
import jax.numpy as jnp
from jax import lax
from jax.experimental import pallas as pl
from jax.experimental.pallas import tpu as pltpu
from jax.sharding import PartitionSpec as P

STEP = 2.0
ROOT_SIX = math.sqrt(6.0)
NODE_TIMES = [(4.0 - ROOT_SIX) / 10.0, (4.0 + ROOT_SIX) / 10.0, 1.0]
COLLOC = [
    [
        (88.0 - 7.0 * ROOT_SIX) / 360.0,
        (296.0 - 169.0 * ROOT_SIX) / 1800.0,
        (-2.0 + 3.0 * ROOT_SIX) / 225.0,
    ],
    [
        (296.0 + 169.0 * ROOT_SIX) / 1800.0,
        (88.0 + 7.0 * ROOT_SIX) / 360.0,
        (-2.0 - 3.0 * ROOT_SIX) / 225.0,
    ],
    [(16.0 - ROOT_SIX) / 36.0, (16.0 + ROOT_SIX) / 36.0, 1.0 / 9.0],
]
MESH = pl.DeviceIdType.MESH
PAD = 8

KAPPA, NODE, START, RES, IMG, GAIN = 0, 1, 4, 5, 9, 13
FIELDS = 15
H_KAPPA, H_NODE, H_RES, H_IMG, H_GAIN = 0, 1, 4, 8, 12
HALOS = 14


def sweep_weight(row, column):
    below = COLLOC[row - 1][column] if row > 0 else 0.0
    return COLLOC[row][column] - below


def node_width(row):
    below = NODE_TIMES[row - 1] if row > 0 else 0.0
    return NODE_TIMES[row] - below


WIDTHS = [STEP * node_width(0), STEP * node_width(1), STEP * node_width(2), STEP]


def chunk_bounds(rows, tile):
    tiles = rows // tile
    parts = min(5, tiles)
    cuts = [tile * (-(-tiles * c // parts)) for c in range(parts + 1)]
    return [(cuts[c], cuts[c + 1] - cuts[c]) for c in range(parts)]


def tile_of(rows, most):
    best = 8
    for size in range(8, most + 1, 8):
        if rows % size == 0:
            best = size
    return best


def kernel(
    slices, slabs, ny, nz,
    start_in, nodes_in, kappa_in,
    fine_out, start_out, coarse_out,
    field, lower, upper, faces, across, result, staged, mail, sums,
    swap_s, swap_r, own_s, halo_s, halo_r, sum_s, sum_r, out_s, out_r, keep_s, end_s, end_r, copy_s,
):
    f32 = jnp.float32
    t = lax.axis_index("tm")
    s = lax.axis_index("space")
    h = lax.rem(s, 2)
    p = lax.div(s, 2)
    pairs = slabs // 2
    half = ny // 2
    win = half + PAD
    other = 1 - h
    partner = s + 1 - 2 * h
    first_row = pl.multiple_of(h * (half - PAD), 8)
    partner_row = pl.multiple_of(other * (half - PAD), 8)
    own = pl.multiple_of(PAD * h, 8)
    mine = pl.multiple_of(h * half, 8)
    has_next = t < slices - 1
    has_prev = t > 0
    has_lower = p > 0
    has_upper = p < pairs - 1
    pending = []

    def start(copy, cond=None):
        if cond is None:
            copy.start()
        else:
            pl.when(cond)(copy.start)
        return copy

    def later(copy, cond=None):
        pending.append((copy, cond))

    def remote(src, dst, send, recv, tm, space):
        return pltpu.make_async_remote_copy(
            src_ref=src, dst_ref=dst, send_sem=send, recv_sem=recv,
            device_id=(tm, space), device_id_type=MESH,
        )

    barrier = pltpu.get_barrier_semaphore()

    def greet(d, carry):
        pl.semaphore_signal(
            barrier, inc=1, device_id=(t, lax.rem(s + d, slabs)), device_id_type=MESH
        )
        return carry

    lax.fori_loop(1, slabs, greet, 0)
    for cond, tm in ((has_next, t + 1), (has_prev, t - 1)):

        @pl.when(cond)
        def _(tm=tm):
            for space in (s, partner):
                pl.semaphore_signal(barrier, inc=1, device_id=(tm, space), device_id_type=MESH)

    sources = [kappa_in.at[0]] + [nodes_in.at[0, j, 0] for j in range(3)] + [start_in.at[0, 0]]
    loads = []
    for k, source in enumerate(sources):
        loads.append(
            start(
                pltpu.make_async_copy(
                    source.at[pl.ds(first_row, win)], field.at[k, h, pl.ds(PAD, win)], own_s.at[k]
                )
            )
        )

    zeros = jnp.zeros((PAD, nz), f32)
    for k in range(FIELDS):
        for slab in range(2):
            field[k, slab, 0:PAD, :] = zeros
            field[k, slab, win + PAD : win + 2 * PAD, :] = zeros

    def clear(ref):
        def body(i, carry):
            for k in range(HALOS):
                ref[k, pl.ds(pl.multiple_of(i * 8, 8), 8), :] = zeros
            return carry

        lax.fori_loop(0, win // 8, body, 0)

    @pl.when(jnp.logical_not(has_lower))
    def _():
        clear(lower)

    @pl.when(jnp.logical_not(has_upper))
    def _():
        clear(upper)

    pl.semaphore_wait(
        barrier,
        slabs - 1 + 2 * has_next.astype(jnp.int32) + 2 * has_prev.astype(jnp.int32),
    )

    tile = tile_of(win, 24)
    bounds = chunk_bounds(win, tile)
    chunks = len(bounds)

    def swap_copy(k, c):
        lo, rows = bounds[c]
        return remote(
            sources[k].at[pl.ds(partner_row + lo, rows)],
            field.at[k, h, pl.ds(PAD + lo, rows)],
            swap_s.at[k, c], swap_r.at[k, c], t, partner,
        )

    def swap_wait(k, c):
        lo, rows = bounds[c]
        dst = field.at[k, other, pl.ds(PAD + lo, rows)]
        remote(dst, dst, swap_s.at[k, c], swap_r.at[k, c], t, partner).wait_recv()

    for c in range(chunks):
        for k in range(5):
            later(start(swap_copy(k, c)))

    def down(f, k, c, lo, rows):
        return remote(
            field.at[f, 0, pl.ds(PAD + lo, rows)], upper.at[k, pl.ds(lo, rows)],
            halo_s.at[k, 0, c], halo_r.at[k, 0, c], t, s - 2,
        )

    def up(f, k, c, lo, rows):
        return remote(
            field.at[f, 1, pl.ds(PAD + lo, rows)], lower.at[k, pl.ds(lo, rows)],
            halo_s.at[k, 1, c], halo_r.at[k, 1, c], t, s + 2,
        )

    def first_hop(k, c, which):
        @pl.when(jnp.logical_and(which == 0, has_lower))
        def _():
            down(k, k, c, *bounds[c]).start()

        @pl.when(jnp.logical_and(which == 1, has_upper))
        def _():
            up(k, k, c, *bounds[c]).start()

    for copy in loads:
        copy.wait()
    for c in range(chunks):
        for k in range(4):
            first_hop(k, c, h)

    def halo_wait(k, c, lo, rows, sides=(0, 1)):
        if 0 in sides:

            @pl.when(has_upper)
            def _():
                remote(
                    upper.at[k, pl.ds(lo, rows)], upper.at[k, pl.ds(lo, rows)],
                    halo_s.at[k, 0, c], halo_r.at[k, 0, c], t, s + 2,
                ).wait_recv()

        if 1 in sides:

            @pl.when(has_lower)
            def _():
                remote(
                    lower.at[k, pl.ds(lo, rows)], lower.at[k, pl.ds(lo, rows)],
                    halo_s.at[k, 1, c], halo_r.at[k, 1, c], t, s - 2,
                ).wait_recv()

    def halo_sent(f, k, c, lo, rows):
        later(down(f, k, c, lo, rows), has_lower)
        later(up(f, k, c, lo, rows), has_upper)

    for k in range(4):
        for c in range(chunks):
            halo_sent(k, k, c, *bounds[c])

    lane = lax.broadcasted_iota(jnp.int32, (tile, nz), 1)

    def loop(rows, size, body, init=0, offset=0):
        def step(i, carry):
            return body(pl.multiple_of(offset + i * size, 8), carry)

        return lax.fori_loop(0, rows // size, step, init)

    def coefficients(b, carry):
        windows = [field[KAPPA, slab, pl.ds(b, tile + 2 * PAD), :] for slab in range(2)]
        centre = [w[PAD : PAD + tile] for w in windows]
        before = 0.5 * (centre[0] + lower[H_KAPPA, pl.ds(b, tile), :])
        between = 0.5 * (centre[0] + centre[1])
        after = 0.5 * (centre[1] + upper[H_KAPPA, pl.ds(b, tile), :])
        across[0, pl.ds(b, tile), :] = before
        across[1, pl.ds(b, tile), :] = between
        across[2, pl.ds(b, tile), :] = after
        ends = [before + between, between + after]
        for slab in range(2):
            w, k = windows[slab], centre[slab]
            above = 0.5 * (k + w[PAD - 1 : PAD - 1 + tile])
            below = 0.5 * (k + w[PAD + 1 : PAD + 1 + tile])
            right = jnp.where(lane == nz - 1, 0.0, pltpu.roll(k, nz - 1, axis=1))
            left = jnp.where(lane == 0, 0.0, pltpu.roll(k, 1, axis=1))
            right_face = 0.5 * (k + right)
            left_face = 0.5 * (k + left)
            faces[0, slab, pl.ds(b, tile), :] = above
            faces[1, slab, pl.ds(b, tile), :] = below
            faces[2, slab, pl.ds(b, tile), :] = jnp.where(lane == nz - 1, 0.0, right_face)
            faces[3, slab, pl.ds(b, tile), :] = ends[slab] + above + below + right_face + left_face
        return carry

    def heat(windows, outer, b, size):
        centre = [w[PAD : PAD + size] for w in windows]
        between = across[1, pl.ds(b, size), :]
        images = []
        for slab in range(2):
            w, v = windows[slab], centre[slab]
            fz = faces[2, slab, pl.ds(b, size), :]
            value = between * centre[1 - slab]
            if outer[slab] is not None:
                value = value + outer[slab]
            value = value + faces[0, slab, pl.ds(b, size), :] * w[PAD - 1 : PAD - 1 + size]
            value = value + faces[1, slab, pl.ds(b, size), :] * w[PAD + 1 : PAD + 1 + size]
            value = value + fz * pltpu.roll(v, nz - 1, axis=1) + pltpu.roll(fz * v, 1, axis=1)
            images.append(value - faces[3, slab, pl.ds(b, size), :] * v)
        return centre, images

    def plain_heat(f, k, b, size):
        windows = [field[f, slab, pl.ds(b, size + 2 * PAD), :] for slab in range(2)]
        outer = (
            across[0, pl.ds(b, size), :] * lower[k, pl.ds(b, size), :],
            across[2, pl.ds(b, size), :] * upper[k, pl.ds(b, size), :],
        )
        return heat(windows, outer, b, size)

    def folded(value):
        return jnp.sum(value.reshape(-1, 8, nz), axis=0)

    def sum_copy(e, d):
        return remote(
            sums.at[e, s], sums.at[e, s], sum_s.at[e, d], sum_r.at[e, d],
            t, lax.rem(s + d, slabs),
        )

    def sum_start(e, parts):
        for row, part in enumerate(parts):
            flat = jnp.sum(part, axis=0, keepdims=True)
            line = flat[:, 0:128]
            for at in range(128, nz, 128):
                line = line + flat[:, at : at + 128]
            sums[e, s, row : row + 1, :] = line

        def body(d, carry):
            sum_copy(e, d).start()
            return carry

        lax.fori_loop(1, slabs, body, 0)

    def sum_wait(e):
        def body(d, carry):
            source = lax.rem(s - d + slabs, slabs)
            remote(
                sums.at[e, source], sums.at[e, source], sum_s.at[e, d], sum_r.at[e, d],
                t, source,
            ).wait_recv()
            return carry

        lax.fori_loop(1, slabs, body, 0)
        total = jnp.sum(sums[e], axis=0)
        total = jnp.sum(total, axis=1, keepdims=True)
        return total[0:1, :], total[1:2, :]

    def halo_send(f, k, c, lo, rows):
        start(down(f, k, c, lo, rows), has_lower)
        start(up(f, k, c, lo, rows), has_upper)
        halo_sent(f, k, c, lo, rows)

    quarter = half // 2
    set_up = own
    set_down = pl.multiple_of(own + quarter, 8)
    pieces_of = (
        ((quarter, quarter + PAD), (0, quarter + PAD)),
        ((0, quarter), (quarter + PAD, quarter)),
    )

    def img_send(m, piece):
        (lo_d, rows_d), (lo_u, rows_u) = pieces_of[piece]
        copies = (
            (down(IMG + m, H_IMG + m, piece, lo_d, rows_d), has_lower),
            (up(IMG + m, H_IMG + m, piece, lo_u, rows_u), has_upper),
        )
        for copy, cond in copies:
            start(copy, cond)
            later(copy, cond)

    def img_wait(m, piece):
        halo_wait(H_IMG + m, piece, *pieces_of[piece][0], (0,))
        halo_wait(H_IMG + m, piece, *pieces_of[piece][1], (1,))

    def product(m):
        def body(b, carry):
            centre, images = plain_heat(RES + m, H_RES + m, b, tile)
            row = lax.broadcasted_iota(jnp.int32, (tile, nz), 0) + b
            inside = jnp.logical_and(row >= own, row < own + half)
            norm, along = carry
            for slab in range(2):
                v = centre[slab]
                z = v - WIDTHS[m] * images[slab]
                field[IMG + m, slab, pl.ds(PAD + b, tile), :] = z
                masked = jnp.where(inside, v, 0.0)
                norm = norm + folded(masked * v)
                along = along + folded(masked * z)
            return norm, along

        nothing = jnp.zeros((8, nz), f32)
        norm, along = loop(win, tile, body, (nothing, nothing))
        sum_start(2 * m, (norm, along))
        img_send(m, 0)

    small = tile_of(quarter, 32)

    def second(m):
        norm_now, along = sum_wait(2 * m)
        step_size = norm_now / along
        img_wait(m, 0)

        def body_of(side):
            ref = lower if side == 0 else upper

            def body(b, carry):
                windows = [
                    field[RES + m, slab, pl.ds(b, small + 2 * PAD), :]
                    - step_size * field[IMG + m, slab, pl.ds(b, small + 2 * PAD), :]
                    for slab in range(2)
                ]
                beside = (
                    ref[H_RES + m, pl.ds(b, small), :]
                    - step_size * ref[H_IMG + m, pl.ds(b, small), :]
                )
                term = 2.0 * across[2 * side, pl.ds(b, small), :] * beside
                outer = (term, None) if side == 0 else (None, term)
                centre, images = heat(windows, outer, b, small)
                norm, along = carry
                for slab in range(2):
                    v = centre[slab]
                    norm = norm + folded(v * v)
                    along = along + folded(v * (v - WIDTHS[m] * images[slab]))
                return norm, along

            return body

        nothing = jnp.zeros((8, nz), f32)
        carry = loop(quarter, small, body_of(0), (nothing, nothing), set_up)
        carry = loop(quarter, small, body_of(1), carry, set_down)
        sum_start(2 * m + 1, carry)
        return norm_now, step_size

    def factors(m, norm_now, step_size):
        norm_next, along = sum_wait(2 * m + 1)
        momentum = norm_next / norm_now
        step_next = norm_next / (along - momentum * norm_next / step_size)
        return step_size + step_next * (1.0 + momentum), step_size * step_next

    def advance(m, scalars):
        on_res, on_img = scalars
        for c in range(chunks):
            halo_wait(H_GAIN + m, c, *spans[c])
        img_wait(m, 1)

        def body(b, carry):
            at = pl.ds(PAD + b, tile)
            rows = pl.ds(b, tile)
            for slab in range(2):
                field[RES + m + 1, slab, at, :] = (
                    field[GAIN + m, slab, at, :]
                    + on_res * field[RES + m, slab, at, :]
                    - on_img * field[IMG + m, slab, at, :]
                )
            for ref in (lower, upper):
                ref[H_RES + m + 1, rows, :] = (
                    ref[H_GAIN + m, rows, :]
                    + on_res * ref[H_RES + m, rows, :]
                    - on_img * ref[H_IMG + m, rows, :]
                )
            return carry

        loop(win, tile, body)

    def coarse_residual():
        def body(b, carry):
            at = pl.ds(PAD + b, tile)
            rows = pl.ds(b, tile)
            for slab in range(2):
                field[RES + 3, slab, at, :] = (
                    field[RES, slab, at, :] + field[GAIN, slab, at, :] + field[GAIN + 1, slab, at, :]
                )
            for ref in (lower, upper):
                ref[H_RES + 3, rows, :] = (
                    ref[H_RES, rows, :] + ref[H_GAIN, rows, :] + ref[H_GAIN + 1, rows, :]
                )
            return carry

        loop(win, tile, body)

    def finish(m, scalars):
        on_res, on_img = scalars
        node = NODE + min(m, 2)

        def body(b, carry):
            for slab in range(2):
                at = pl.ds(PAD + b, small)
                result[m, slab, pl.ds(b, small), :] = (
                    field[node, slab, at, :]
                    + on_res * field[RES + m, slab, at, :]
                    - on_img * field[IMG + m, slab, at, :]
                )
            return carry

        loop(half, small, body, 0, own)

    def residuals(b, carry):
        images = [plain_heat(NODE + j, H_NODE + j, b, tile)[1] for j in range(3)]
        at = pl.ds(PAD + b, tile)
        for slab in range(2):
            nodes = [field[NODE + j, slab, at, :] for j in range(3)]
            ahead = [field[START, slab, at, :]] + nodes
            for row, f in enumerate((RES, GAIN, GAIN + 1)):
                value = ahead[row] - nodes[row]
                for j in range(3):
                    value = value + (STEP * sweep_weight(row, j)) * images[j][slab]
                field[f, slab, at, :] = value
        return carry

    spans = []
    for c, (lo, rows) in enumerate(bounds):
        begin = lo - tile if c else 0
        end = lo + rows - (tile if c < chunks - 1 else 0)
        spans.append((begin, end - begin))

    def begin_rows(c):
        for k in range(4):
            halo_wait(k, c, *bounds[c])
        lo, rows = spans[c]
        loop(rows, tile, coefficients, 0, lo)
        loop(rows, tile, residuals, 0, lo)
        halo_send(RES, H_RES, c, lo, rows)
        if c == 0:
            halo_send(GAIN, H_GAIN, c, lo, rows)

    order = [(k, c) for c in range(chunks) for k in range(5)]
    ready = {}
    for c in range(chunks):
        ready[min(5 * c + 6, len(order) - 1)] = c
    for n, (k, c) in enumerate(order):
        swap_wait(k, c)
        if k < 4:
            first_hop(k, c, other)
        if n in ready:
            begin_rows(ready[n])
    for c in range(1, chunks - 1):
        halo_send(GAIN, H_GAIN, c, *spans[c])

    def give_back(m):
        later(
            start(
                remote(
                    result.at[m, other, pl.ds(own, half)], fine_out.at[0, m, 0, pl.ds(mine, half)],
                    out_s.at[m], out_r.at[m], t, partner,
                )
            )
        )
        keep = pltpu.make_async_copy(
            result.at[m, h, pl.ds(own, half)], fine_out.at[0, m, 0, pl.ds(mine, half)], keep_s.at[m]
        )
        keep.start()
        return keep

    theirs = pl.multiple_of(other * half, 8)

    @pl.when(jnp.logical_not(has_prev))
    def _():
        pltpu.make_async_copy(start_in.at[0, 0], staged, copy_s.at[0]).start()

    for c in range(chunks):
        halo_wait(H_RES, c, *spans[c])
    product(0)
    halo_send(GAIN, H_GAIN, chunks - 1, *spans[chunks - 1])
    scalars = second(0)
    img_send(0, 1)
    halo_send(GAIN + 1, H_GAIN + 1, 0, *spans[0])
    update = factors(0, *scalars)
    advance(0, update)
    product(1)
    for c in range(1, chunks - 1):
        halo_send(GAIN + 1, H_GAIN + 1, c, *spans[c])
    finish(0, update)
    keeps = [give_back(0)]
    @pl.when(jnp.logical_not(has_prev))
    def _():
        pltpu.make_async_copy(start_in.at[0, 0], staged, copy_s.at[0]).wait()
        first = pltpu.make_async_copy(staged, start_out.at[0, 0], copy_s.at[0])
        second_copy = pltpu.make_async_copy(staged, coarse_out.at[0, 0], copy_s.at[1])
        first.start()
        second_copy.start()
        first.wait()
        second_copy.wait()

    scalars = second(1)
    img_send(1, 1)
    halo_send(GAIN + 1, H_GAIN + 1, chunks - 1, *spans[chunks - 1])
    update = factors(1, *scalars)
    advance(1, update)
    product(2)
    coarse_residual()
    product(3)
    scalars = second(2)
    finish(1, update)
    keeps.append(give_back(1))
    scalars_coarse = second(3)
    finish(2, factors(2, *scalars))
    pieces = 2
    piece = half // pieces
    for c in range(pieces):
        later(
            start(
                remote(
                    result.at[2, other, pl.ds(own + c * piece, piece)],
                    mail.at[pl.ds(c * piece, piece)],
                    out_s.at[2 + c], out_r.at[2 + c], t, partner,
                )
            )
        )
    for c in range(pieces):
        rows = pl.ds(mine + c * piece, piece)
        src = result.at[2, h, pl.ds(own + c * piece, piece)]
        copy = remote(src, start_out.at[0, 0, rows], end_s.at[2 + c], end_r.at[2 + c], t + 1, s)
        start(copy, has_next)
        later(copy, has_next)
        keep = pltpu.make_async_copy(src, fine_out.at[0, 2, 0, rows], keep_s.at[2 + c])
        keep.start()
        keeps.append(keep)
    finish(3, factors(3, *scalars_coarse))

    def coarse_copies():
        return [
            remote(
                result.at[3, h, pl.ds(own, half)], coarse_out.at[0, 0, pl.ds(mine, half)],
                end_s.at[0], end_r.at[0], t + 1, s,
            ),
            remote(
                result.at[3, other, pl.ds(own, half)], coarse_out.at[0, 0, pl.ds(mine, half)],
                end_s.at[1], end_r.at[1], t + 1, partner,
            ),
        ]

    for copy in coarse_copies():
        start(copy, has_next)
        later(copy, has_next)

    for c in range(pieces):
        rows = pl.ds(theirs + c * piece, piece)
        src = mail.at[pl.ds(c * piece, piece)]
        remote(src, src, out_s.at[2 + c], out_r.at[2 + c], t, partner).wait_recv()
        copy = remote(
            src, start_out.at[0, 0, rows],
            end_s.at[2 + pieces + c], end_r.at[2 + pieces + c], t + 1, s,
        )
        start(copy, has_next)
        later(copy, has_next)
        keep = pltpu.make_async_copy(src, fine_out.at[0, 2, 0, rows], keep_s.at[2 + pieces + c])
        keep.start()
        keeps.append(keep)

    for m in range(2):
        dst = fine_out.at[0, m, 0, pl.ds(theirs, half)]
        remote(dst, dst, out_s.at[m], out_r.at[m], t, partner).wait_recv()

    @pl.when(has_prev)
    def _():
        for k in range(2):
            at = mine if k == 0 else theirs
            dst = coarse_out.at[0, 0, pl.ds(at, half)]
            remote(dst, dst, end_s.at[k], end_r.at[k], t - 1, s).wait_recv()
        for k in range(2):
            at = mine if k == 0 else theirs
            for c in range(pieces):
                dst = start_out.at[0, 0, pl.ds(at + c * piece, piece)]
                e = 2 + k * pieces + c
                remote(dst, dst, end_s.at[e], end_r.at[e], t - 1, s).wait_recv()

    for keep in keeps:
        keep.wait()
    for copy, cond in pending:
        if cond is None:
            copy.wait_send()
        else:
            pl.when(cond)(copy.wait_send)

    def drain(d, carry):
        for e in range(8):
            sum_copy(e, d).wait_send()
        return carry

    lax.fori_loop(1, slabs, drain, 0)


def solution(mesh):
    slices, slabs = mesh.shape["tm"], mesh.shape["space"]

    def on_device(start_value, old_nodes, diffusivity):
        ny, nz = start_value.shape[2:]
        half = ny // 2
        win = half + PAD
        chunks = len(chunk_bounds(win, tile_of(win, 24)))
        vmem = lambda *shape: pltpu.VMEM(shape, jnp.float32)
        dma = lambda *shape: pltpu.SemaphoreType.DMA(shape)

        def body(*refs):
            kernel(slices, slabs, ny, nz, *refs)

        return pl.pallas_call(
            body,
            out_shape=(
                jax.ShapeDtypeStruct(old_nodes.shape, jnp.float32),
                jax.ShapeDtypeStruct(start_value.shape, jnp.float32),
                jax.ShapeDtypeStruct(start_value.shape, jnp.float32),
            ),
            in_specs=[pl.BlockSpec(memory_space=pl.ANY)] * 3,
            out_specs=(pl.BlockSpec(memory_space=pl.ANY),) * 3,
            scratch_shapes=[
                vmem(FIELDS, 2, win + 2 * PAD, nz),
                vmem(HALOS, win, nz),
                vmem(HALOS, win, nz),
                vmem(4, 2, win, nz),
                vmem(3, win, nz),
                vmem(4, 2, win, nz),
                vmem(ny, nz),
                vmem(half, nz),
                vmem(8, slabs, 2, 128),
                dma(5, chunks), dma(5, chunks), dma(5),
                dma(HALOS, 2, chunks), dma(HALOS, 2, chunks),
                dma(8, slabs), dma(8, slabs),
                dma(4), dma(4), dma(6), dma(6), dma(6), dma(2),
            ],
            compiler_params=pltpu.CompilerParams(
                collective_id=0, has_side_effects=True, vmem_limit_bytes=60 * 1024 * 1024
            ),
            name="pfasst",
        )(start_value, old_nodes, diffusivity)

    in_specs = (
        P("tm", "space", None, None),
        P("tm", None, "space", None, None),
        P("space", None, None),
    )
    out_specs = (
        P("tm", None, "space", None, None),
        P("tm", "space", None, None),
        P("tm", "space", None, None),
    )
    return jax.shard_map(
        on_device, mesh=mesh, in_specs=in_specs, out_specs=out_specs, check_vma=False
    )
```

```python
import math

import jax
import jax.numpy as jnp
from jax import lax
from jax.experimental import pallas as pl
from jax.experimental.pallas import tpu as pltpu
from jax.sharding import PartitionSpec as P

STEP = 2.0
ROOT_SIX = math.sqrt(6.0)
NODE_TIMES = [(4.0 - ROOT_SIX) / 10.0, (4.0 + ROOT_SIX) / 10.0, 1.0]
COLLOC = [
    [
        (88.0 - 7.0 * ROOT_SIX) / 360.0,
        (296.0 - 169.0 * ROOT_SIX) / 1800.0,
        (-2.0 + 3.0 * ROOT_SIX) / 225.0,
    ],
    [
        (296.0 + 169.0 * ROOT_SIX) / 1800.0,
        (88.0 + 7.0 * ROOT_SIX) / 360.0,
        (-2.0 - 3.0 * ROOT_SIX) / 225.0,
    ],
    [(16.0 - ROOT_SIX) / 36.0, (16.0 + ROOT_SIX) / 36.0, 1.0 / 9.0],
]
MESH = pl.DeviceIdType.MESH
PAD = 8

KAPPA, NODE, START, RES, IMG, GAIN = 0, 1, 4, 5, 9, 13
FIELDS = 15
H_KAPPA, H_NODE, H_RES, H_IMG, H_GAIN = 0, 1, 4, 8, 12
HALOS = 14


def sweep_weight(row, column):
    below = COLLOC[row - 1][column] if row > 0 else 0.0
    return COLLOC[row][column] - below


def node_width(row):
    below = NODE_TIMES[row - 1] if row > 0 else 0.0
    return NODE_TIMES[row] - below


WIDTHS = [STEP * node_width(0), STEP * node_width(1), STEP * node_width(2), STEP]


def chunk_bounds(rows, tile):
    tiles = rows // tile
    parts = min(5, tiles)
    cuts = [tile * (-(-tiles * c // parts)) for c in range(parts + 1)]
    return [(cuts[c], cuts[c + 1] - cuts[c]) for c in range(parts)]


def tile_of(rows, most):
    best = 8
    for size in range(8, most + 1, 8):
        if rows % size == 0:
            best = size
    return best


def kernel(
    slices, slabs, ny, nz,
    start_in, nodes_in, kappa_in,
    fine_out, start_out, coarse_out,
    field, lower, upper, faces, across, result, staged, mail, sums,
    swap_s, swap_r, own_s, halo_s, halo_r, sum_s, sum_r, out_s, out_r, keep_s, end_s, end_r, copy_s,
):
    f32 = jnp.float32
    t = lax.axis_index("tm")
    s = lax.axis_index("space")
    h = lax.rem(s, 2)
    p = lax.div(s, 2)
    pairs = slabs // 2
    half = ny // 2
    win = half + PAD
    other = 1 - h
    partner = s + 1 - 2 * h
    first_row = pl.multiple_of(h * (half - PAD), 8)
    partner_row = pl.multiple_of(other * (half - PAD), 8)
    own = pl.multiple_of(PAD * h, 8)
    mine = pl.multiple_of(h * half, 8)
    has_next = t < slices - 1
    has_prev = t > 0
    has_lower = p > 0
    has_upper = p < pairs - 1
    pending = []

    def start(copy, cond=None):
        if cond is None:
            copy.start()
        else:
            pl.when(cond)(copy.start)
        return copy

    def later(copy, cond=None):
        pending.append((copy, cond))

    def remote(src, dst, send, recv, tm, space):
        return pltpu.make_async_remote_copy(
            src_ref=src, dst_ref=dst, send_sem=send, recv_sem=recv,
            device_id=(tm, space), device_id_type=MESH,
        )

    barrier = pltpu.get_barrier_semaphore()

    def greet(d, carry):
        pl.semaphore_signal(
            barrier, inc=1, device_id=(t, lax.rem(s + d, slabs)), device_id_type=MESH
        )
        return carry

    lax.fori_loop(1, slabs, greet, 0)
    for cond, tm in ((has_next, t + 1), (has_prev, t - 1)):

        @pl.when(cond)
        def _(tm=tm):
            for space in (s, partner):
                pl.semaphore_signal(barrier, inc=1, device_id=(tm, space), device_id_type=MESH)

    sources = [kappa_in.at[0]] + [nodes_in.at[0, j, 0] for j in range(3)] + [start_in.at[0, 0]]
    loads = []
    for k, source in enumerate(sources):
        loads.append(
            start(
                pltpu.make_async_copy(
                    source.at[pl.ds(first_row, win)], field.at[k, h, pl.ds(PAD, win)], own_s.at[k]
                )
            )
        )

    zeros = jnp.zeros((PAD, nz), f32)
    for k in range(FIELDS):
        for slab in range(2):
            field[k, slab, 0:PAD, :] = zeros
            field[k, slab, win + PAD : win + 2 * PAD, :] = zeros

    def clear(ref):
        def body(i, carry):
            for k in range(HALOS):
                ref[k, pl.ds(pl.multiple_of(i * 8, 8), 8), :] = zeros
            return carry

        lax.fori_loop(0, win // 8, body, 0)

    @pl.when(jnp.logical_not(has_lower))
    def _():
        clear(lower)

    @pl.when(jnp.logical_not(has_upper))
    def _():
        clear(upper)

    pl.semaphore_wait(
        barrier,
        slabs - 1 + 2 * has_next.astype(jnp.int32) + 2 * has_prev.astype(jnp.int32),
    )

    tile = tile_of(win, 24)
    bounds = chunk_bounds(win, tile)
    chunks = len(bounds)

    def swap_copy(k, c):
        lo, rows = bounds[c]
        return remote(
            sources[k].at[pl.ds(partner_row + lo, rows)],
            field.at[k, h, pl.ds(PAD + lo, rows)],
            swap_s.at[k, c], swap_r.at[k, c], t, partner,
        )

    def swap_wait(k, c):
        lo, rows = bounds[c]
        dst = field.at[k, other, pl.ds(PAD + lo, rows)]
        remote(dst, dst, swap_s.at[k, c], swap_r.at[k, c], t, partner).wait_recv()

    for c in range(chunks):
        for k in range(5):
            later(start(swap_copy(k, c)))

    def down(f, k, c, lo, rows):
        return remote(
            field.at[f, 0, pl.ds(PAD + lo, rows)], upper.at[k, pl.ds(lo, rows)],
            halo_s.at[k, 0, c], halo_r.at[k, 0, c], t, s - 2,
        )

    def up(f, k, c, lo, rows):
        return remote(
            field.at[f, 1, pl.ds(PAD + lo, rows)], lower.at[k, pl.ds(lo, rows)],
            halo_s.at[k, 1, c], halo_r.at[k, 1, c], t, s + 2,
        )

    def first_hop(k, c, which):
        @pl.when(jnp.logical_and(which == 0, has_lower))
        def _():
            down(k, k, c, *bounds[c]).start()

        @pl.when(jnp.logical_and(which == 1, has_upper))
        def _():
            up(k, k, c, *bounds[c]).start()

    for copy in loads:
        copy.wait()
    for c in range(chunks):
        for k in range(4):
            first_hop(k, c, h)

    def halo_wait(k, c, lo, rows, sides=(0, 1)):
        if 0 in sides:

            @pl.when(has_upper)
            def _():
                remote(
                    upper.at[k, pl.ds(lo, rows)], upper.at[k, pl.ds(lo, rows)],
                    halo_s.at[k, 0, c], halo_r.at[k, 0, c], t, s + 2,
                ).wait_recv()

        if 1 in sides:

            @pl.when(has_lower)
            def _():
                remote(
                    lower.at[k, pl.ds(lo, rows)], lower.at[k, pl.ds(lo, rows)],
                    halo_s.at[k, 1, c], halo_r.at[k, 1, c], t, s - 2,
                ).wait_recv()

    def halo_sent(f, k, c, lo, rows):
        later(down(f, k, c, lo, rows), has_lower)
        later(up(f, k, c, lo, rows), has_upper)

    for k in range(4):
        for c in range(chunks):
            halo_sent(k, k, c, *bounds[c])

    lane = lax.broadcasted_iota(jnp.int32, (tile, nz), 1)

    def loop(rows, size, body, init=0, offset=0):
        def step(i, carry):
            return body(pl.multiple_of(offset + i * size, 8), carry)

        return lax.fori_loop(0, rows // size, step, init)

    def coefficients(b, carry):
        windows = [field[KAPPA, slab, pl.ds(b, tile + 2 * PAD), :] for slab in range(2)]
        centre = [w[PAD : PAD + tile] for w in windows]
        before = 0.5 * (centre[0] + lower[H_KAPPA, pl.ds(b, tile), :])
        between = 0.5 * (centre[0] + centre[1])
        after = 0.5 * (centre[1] + upper[H_KAPPA, pl.ds(b, tile), :])
        across[0, pl.ds(b, tile), :] = before
        across[1, pl.ds(b, tile), :] = between
        across[2, pl.ds(b, tile), :] = after
        ends = [before + between, between + after]
        for slab in range(2):
            w, k = windows[slab], centre[slab]
            above = 0.5 * (k + w[PAD - 1 : PAD - 1 + tile])
            below = 0.5 * (k + w[PAD + 1 : PAD + 1 + tile])
            right = jnp.where(lane == nz - 1, 0.0, pltpu.roll(k, nz - 1, axis=1))
            left = jnp.where(lane == 0, 0.0, pltpu.roll(k, 1, axis=1))
            right_face = 0.5 * (k + right)
            left_face = 0.5 * (k + left)
            faces[0, slab, pl.ds(b, tile), :] = above
            faces[1, slab, pl.ds(b, tile), :] = below
            faces[2, slab, pl.ds(b, tile), :] = jnp.where(lane == nz - 1, 0.0, right_face)
            faces[3, slab, pl.ds(b, tile), :] = ends[slab] + above + below + right_face + left_face
        return carry

    def heat(windows, outer, b, size):
        centre = [w[PAD : PAD + size] for w in windows]
        between = across[1, pl.ds(b, size), :]
        images = []
        for slab in range(2):
            w, v = windows[slab], centre[slab]
            fz = faces[2, slab, pl.ds(b, size), :]
            value = between * centre[1 - slab]
            if outer[slab] is not None:
                value = value + outer[slab]
            value = value + faces[0, slab, pl.ds(b, size), :] * w[PAD - 1 : PAD - 1 + size]
            value = value + faces[1, slab, pl.ds(b, size), :] * w[PAD + 1 : PAD + 1 + size]
            value = value + fz * pltpu.roll(v, nz - 1, axis=1) + pltpu.roll(fz * v, 1, axis=1)
            images.append(value - faces[3, slab, pl.ds(b, size), :] * v)
        return centre, images

    def plain_heat(f, k, b, size):
        windows = [field[f, slab, pl.ds(b, size + 2 * PAD), :] for slab in range(2)]
        outer = (
            across[0, pl.ds(b, size), :] * lower[k, pl.ds(b, size), :],
            across[2, pl.ds(b, size), :] * upper[k, pl.ds(b, size), :],
        )
        return heat(windows, outer, b, size)

    def folded(value):
        return jnp.sum(value.reshape(-1, 8, nz), axis=0)

    def sum_copy(e, d):
        return remote(
            sums.at[e, s], sums.at[e, s], sum_s.at[e, d], sum_r.at[e, d],
            t, lax.rem(s + d, slabs),
        )

    def sum_start(e, parts):
        for row, part in enumerate(parts):
            flat = jnp.sum(part, axis=0, keepdims=True)
            line = flat[:, 0:128]
            for at in range(128, nz, 128):
                line = line + flat[:, at : at + 128]
            sums[e, s, row : row + 1, :] = line

        def body(d, carry):
            sum_copy(e, d).start()
            return carry

        lax.fori_loop(1, slabs, body, 0)

    def sum_wait(e):
        def body(d, carry):
            source = lax.rem(s - d + slabs, slabs)
            remote(
                sums.at[e, source], sums.at[e, source], sum_s.at[e, d], sum_r.at[e, d],
                t, source,
            ).wait_recv()
            return carry

        lax.fori_loop(1, slabs, body, 0)
        total = jnp.sum(sums[e], axis=0)
        total = jnp.sum(total, axis=1, keepdims=True)
        return total[0:1, :], total[1:2, :]

    def halo_send(f, k, c, lo, rows):
        start(down(f, k, c, lo, rows), has_lower)
        start(up(f, k, c, lo, rows), has_upper)
        halo_sent(f, k, c, lo, rows)

    quarter = half // 2
    set_up = own
    set_down = pl.multiple_of(own + quarter, 8)
    pieces_of = (
        ((quarter, quarter + PAD), (0, quarter + PAD)),
        ((0, quarter), (quarter + PAD, quarter)),
    )

    def img_send(m, piece):
        (lo_d, rows_d), (lo_u, rows_u) = pieces_of[piece]
        copies = (
            (down(IMG + m, H_IMG + m, piece, lo_d, rows_d), has_lower),
            (up(IMG + m, H_IMG + m, piece, lo_u, rows_u), has_upper),
        )
        for copy, cond in copies:
            start(copy, cond)
            later(copy, cond)

    def img_wait(m, piece):
        halo_wait(H_IMG + m, piece, *pieces_of[piece][0], (0,))
        halo_wait(H_IMG + m, piece, *pieces_of[piece][1], (1,))

    def product(m):
        def body(b, carry):
            centre, images = plain_heat(RES + m, H_RES + m, b, tile)
            row = lax.broadcasted_iota(jnp.int32, (tile, nz), 0) + b
            inside = jnp.logical_and(row >= own, row < own + half)
            norm, along = carry
            for slab in range(2):
                v = centre[slab]
                z = v - WIDTHS[m] * images[slab]
                field[IMG + m, slab, pl.ds(PAD + b, tile), :] = z
                masked = jnp.where(inside, v, 0.0)
                norm = norm + folded(masked * v)
                along = along + folded(masked * z)
            return norm, along

        nothing = jnp.zeros((8, nz), f32)
        norm, along = loop(win, tile, body, (nothing, nothing))
        sum_start(2 * m, (norm, along))
        img_send(m, 0)

    small = tile_of(quarter, 32)

    def second(m):
        norm_now, along = sum_wait(2 * m)
        step_size = norm_now / along
        img_wait(m, 0)

        def body_of(side):
            ref = lower if side == 0 else upper

            def body(b, carry):
                windows = [
                    field[RES + m, slab, pl.ds(b, small + 2 * PAD), :]
                    - step_size * field[IMG + m, slab, pl.ds(b, small + 2 * PAD), :]
                    for slab in range(2)
                ]
                beside = (
                    ref[H_RES + m, pl.ds(b, small), :]
                    - step_size * ref[H_IMG + m, pl.ds(b, small), :]
                )
                term = 2.0 * across[2 * side, pl.ds(b, small), :] * beside
                outer = (term, None) if side == 0 else (None, term)
                centre, images = heat(windows, outer, b, small)
                norm, along = carry
                for slab in range(2):
                    v = centre[slab]
                    norm = norm + folded(v * v)
                    along = along + folded(v * (v - WIDTHS[m] * images[slab]))
                return norm, along

            return body

        nothing = jnp.zeros((8, nz), f32)
        carry = loop(quarter, small, body_of(0), (nothing, nothing), set_up)
        carry = loop(quarter, small, body_of(1), carry, set_down)
        sum_start(2 * m + 1, carry)
        return norm_now, step_size

    def factors(m, norm_now, step_size):
        norm_next, along = sum_wait(2 * m + 1)
        momentum = norm_next / norm_now
        step_next = norm_next / (along - momentum * norm_next / step_size)
        return step_size + step_next * (1.0 + momentum), step_size * step_next

    def advance(m, scalars):
        on_res, on_img = scalars
        for c in range(chunks):
            halo_wait(H_GAIN + m, c, *spans[c])
        img_wait(m, 1)

        def body(b, carry):
            at = pl.ds(PAD + b, tile)
            rows = pl.ds(b, tile)
            for slab in range(2):
                field[RES + m + 1, slab, at, :] = (
                    field[GAIN + m, slab, at, :]
                    + on_res * field[RES + m, slab, at, :]
                    - on_img * field[IMG + m, slab, at, :]
                )
            for ref in (lower, upper):
                ref[H_RES + m + 1, rows, :] = (
                    ref[H_GAIN + m, rows, :]
                    + on_res * ref[H_RES + m, rows, :]
                    - on_img * ref[H_IMG + m, rows, :]
                )
            return carry

        loop(win, tile, body)

    def coarse_residual():
        def body(b, carry):
            at = pl.ds(PAD + b, tile)
            rows = pl.ds(b, tile)
            for slab in range(2):
                field[RES + 3, slab, at, :] = (
                    field[RES, slab, at, :] + field[GAIN, slab, at, :] + field[GAIN + 1, slab, at, :]
                )
            for ref in (lower, upper):
                ref[H_RES + 3, rows, :] = (
                    ref[H_RES, rows, :] + ref[H_GAIN, rows, :] + ref[H_GAIN + 1, rows, :]
                )
            return carry

        loop(win, tile, body)

    def finish(m, scalars):
        on_res, on_img = scalars
        node = NODE + min(m, 2)

        def body(b, carry):
            for slab in range(2):
                at = pl.ds(PAD + b, small)
                result[m, slab, pl.ds(b, small), :] = (
                    field[node, slab, at, :]
                    + on_res * field[RES + m, slab, at, :]
                    - on_img * field[IMG + m, slab, at, :]
                )
            return carry

        loop(half, small, body, 0, own)

    def residuals(b, carry):
        images = [plain_heat(NODE + j, H_NODE + j, b, tile)[1] for j in range(3)]
        at = pl.ds(PAD + b, tile)
        for slab in range(2):
            nodes = [field[NODE + j, slab, at, :] for j in range(3)]
            ahead = [field[START, slab, at, :]] + nodes
            for row, f in enumerate((RES, GAIN, GAIN + 1)):
                value = ahead[row] - nodes[row]
                for j in range(3):
                    value = value + (STEP * sweep_weight(row, j)) * images[j][slab]
                field[f, slab, at, :] = value
        return carry

    spans = []
    for c, (lo, rows) in enumerate(bounds):
        begin = lo - tile if c else 0
        end = lo + rows - (tile if c < chunks - 1 else 0)
        spans.append((begin, end - begin))

    def begin_rows(c):
        for k in range(4):
            halo_wait(k, c, *bounds[c])
        lo, rows = spans[c]
        loop(rows, tile, coefficients, 0, lo)
        loop(rows, tile, residuals, 0, lo)
        halo_send(RES, H_RES, c, lo, rows)
        if c == 0:
            halo_send(GAIN, H_GAIN, c, lo, rows)

    order = [(k, c) for c in range(chunks) for k in range(5)]
    ready = {}
    for c in range(chunks):
        ready[min(5 * c + 6, len(order) - 1)] = c
    for n, (k, c) in enumerate(order):
        swap_wait(k, c)
        if k < 4:
            first_hop(k, c, other)
        if n in ready:
            begin_rows(ready[n])
    for c in range(1, chunks - 1):
        halo_send(GAIN, H_GAIN, c, *spans[c])

    def give_back(m):
        later(
            start(
                remote(
                    result.at[m, other, pl.ds(own, half)], fine_out.at[0, m, 0, pl.ds(mine, half)],
                    out_s.at[m], out_r.at[m], t, partner,
                )
            )
        )
        keep = pltpu.make_async_copy(
            result.at[m, h, pl.ds(own, half)], fine_out.at[0, m, 0, pl.ds(mine, half)], keep_s.at[m]
        )
        keep.start()
        return keep

    theirs = pl.multiple_of(other * half, 8)

    @pl.when(jnp.logical_not(has_prev))
    def _():
        pltpu.make_async_copy(start_in.at[0, 0], staged, copy_s.at[0]).start()

    for c in range(chunks):
        halo_wait(H_RES, c, *spans[c])
    product(0)
    halo_send(GAIN, H_GAIN, chunks - 1, *spans[chunks - 1])
    scalars = second(0)
    img_send(0, 1)
    halo_send(GAIN + 1, H_GAIN + 1, 0, *spans[0])
    update = factors(0, *scalars)
    advance(0, update)
    product(1)
    for c in range(1, chunks - 1):
        halo_send(GAIN + 1, H_GAIN + 1, c, *spans[c])
    finish(0, update)
    keeps = [give_back(0)]
    @pl.when(jnp.logical_not(has_prev))
    def _():
        pltpu.make_async_copy(start_in.at[0, 0], staged, copy_s.at[0]).wait()
        first = pltpu.make_async_copy(staged, start_out.at[0, 0], copy_s.at[0])
        second_copy = pltpu.make_async_copy(staged, coarse_out.at[0, 0], copy_s.at[1])
        first.start()
        second_copy.start()
        first.wait()
        second_copy.wait()

    scalars = second(1)
    img_send(1, 1)
    halo_send(GAIN + 1, H_GAIN + 1, chunks - 1, *spans[chunks - 1])
    update = factors(1, *scalars)
    advance(1, update)
    product(2)
    coarse_residual()
    product(3)
    scalars = second(2)
    finish(1, update)
    keeps.append(give_back(1))
    scalars_coarse = second(3)
    finish(2, factors(2, *scalars))
    pieces = 4
    piece = half // pieces
    for c in range(pieces):
        later(
            start(
                remote(
                    result.at[2, other, pl.ds(own + c * piece, piece)],
                    mail.at[pl.ds(c * piece, piece)],
                    out_s.at[2 + c], out_r.at[2 + c], t, partner,
                )
            )
        )
    for c in range(pieces):
        rows = pl.ds(mine + c * piece, piece)
        src = result.at[2, h, pl.ds(own + c * piece, piece)]
        copy = remote(src, start_out.at[0, 0, rows], end_s.at[2 + c], end_r.at[2 + c], t + 1, s)
        start(copy, has_next)
        later(copy, has_next)
        keep = pltpu.make_async_copy(src, fine_out.at[0, 2, 0, rows], keep_s.at[2 + c])
        keep.start()
        keeps.append(keep)
    finish(3, factors(3, *scalars_coarse))

    def coarse_copies():
        return [
            remote(
                result.at[3, h, pl.ds(own, half)], coarse_out.at[0, 0, pl.ds(mine, half)],
                end_s.at[0], end_r.at[0], t + 1, s,
            ),
            remote(
                result.at[3, other, pl.ds(own, half)], coarse_out.at[0, 0, pl.ds(mine, half)],
                end_s.at[1], end_r.at[1], t + 1, partner,
            ),
        ]

    for copy in coarse_copies():
        start(copy, has_next)
        later(copy, has_next)

    for c in range(pieces):
        rows = pl.ds(theirs + c * piece, piece)
        src = mail.at[pl.ds(c * piece, piece)]
        remote(src, src, out_s.at[2 + c], out_r.at[2 + c], t, partner).wait_recv()
        copy = remote(
            src, start_out.at[0, 0, rows],
            end_s.at[2 + pieces + c], end_r.at[2 + pieces + c], t + 1, s,
        )
        start(copy, has_next)
        later(copy, has_next)
        keep = pltpu.make_async_copy(src, fine_out.at[0, 2, 0, rows], keep_s.at[2 + pieces + c])
        keep.start()
        keeps.append(keep)

    for m in range(2):
        dst = fine_out.at[0, m, 0, pl.ds(theirs, half)]
        remote(dst, dst, out_s.at[m], out_r.at[m], t, partner).wait_recv()

    @pl.when(has_prev)
    def _():
        for k in range(2):
            at = mine if k == 0 else theirs
            dst = coarse_out.at[0, 0, pl.ds(at, half)]
            remote(dst, dst, end_s.at[k], end_r.at[k], t - 1, s).wait_recv()
        for k in range(2):
            at = mine if k == 0 else theirs
            for c in range(pieces):
                dst = start_out.at[0, 0, pl.ds(at + c * piece, piece)]
                e = 2 + k * pieces + c
                remote(dst, dst, end_s.at[e], end_r.at[e], t - 1, s).wait_recv()

    for keep in keeps:
        keep.wait()
    for copy, cond in pending:
        if cond is None:
            copy.wait_send()
        else:
            pl.when(cond)(copy.wait_send)

    def drain(d, carry):
        for e in range(8):
            sum_copy(e, d).wait_send()
        return carry

    lax.fori_loop(1, slabs, drain, 0)


def solution(mesh):
    slices, slabs = mesh.shape["tm"], mesh.shape["space"]

    def on_device(start_value, old_nodes, diffusivity):
        ny, nz = start_value.shape[2:]
        half = ny // 2
        win = half + PAD
        chunks = len(chunk_bounds(win, tile_of(win, 24)))
        vmem = lambda *shape: pltpu.VMEM(shape, jnp.float32)
        dma = lambda *shape: pltpu.SemaphoreType.DMA(shape)

        def body(*refs):
            kernel(slices, slabs, ny, nz, *refs)

        return pl.pallas_call(
            body,
            out_shape=(
                jax.ShapeDtypeStruct(old_nodes.shape, jnp.float32),
                jax.ShapeDtypeStruct(start_value.shape, jnp.float32),
                jax.ShapeDtypeStruct(start_value.shape, jnp.float32),
            ),
            in_specs=[pl.BlockSpec(memory_space=pl.ANY)] * 3,
            out_specs=(pl.BlockSpec(memory_space=pl.ANY),) * 3,
            scratch_shapes=[
                vmem(FIELDS, 2, win + 2 * PAD, nz),
                vmem(HALOS, win, nz),
                vmem(HALOS, win, nz),
                vmem(4, 2, win, nz),
                vmem(3, win, nz),
                vmem(4, 2, win, nz),
                vmem(ny, nz),
                vmem(half, nz),
                vmem(8, slabs, 2, 128),
                dma(5, chunks), dma(5, chunks), dma(5),
                dma(HALOS, 2, chunks), dma(HALOS, 2, chunks),
                dma(8, slabs), dma(8, slabs),
                dma(6), dma(6), dma(10), dma(10), dma(10), dma(2),
            ],
            compiler_params=pltpu.CompilerParams(
                collective_id=0, has_side_effects=True, vmem_limit_bytes=60 * 1024 * 1024
            ),
            name="pfasst",
        )(start_value, old_nodes, diffusivity)

    in_specs = (
        P("tm", "space", None, None),
        P("tm", None, "space", None, None),
        P("space", None, None),
    )
    out_specs = (
        P("tm", None, "space", None, None),
        P("tm", "space", None, None),
        P("tm", "space", None, None),
    )
    return jax.shard_map(
        on_device, mesh=mesh, in_specs=in_specs, out_specs=out_specs, check_vma=False
    )
```
